512 devices in a mesh: pipe: 16 (over z, core), ctx: 32 (over y, x).
Axes of the slice: x: 4, y: 8, z: 8, core: 2. Of those that a mesh axis runs over, the one named last changes fastest.
Arguments:
- states: bfloat16 [16, 4096, 2048], P('pipe', 'ctx'), may hold values from -6 to 6
- norm_gain: float32 [16, 2048], P('pipe'), may hold values from 0.25 to 1.75
- w_in: bfloat16 [16, 2048, 1536], P('pipe', 'ctx'), may hold values from -1 to 1
- w_out: bfloat16 [16, 1024, 2048], P('pipe', 'ctx'), may hold values from -0.1875 to 0.1875
- lengths: int32 [16, 8], replicated, may hold values from 1 to 1024, 4096 in all within a row
Outputs:
- moved: bfloat16 [16, 4096, 2048], P('pipe', 'ctx')
The draws below stay inside these ranges and needn't reach their ends.
Inputs may be any that keep to these rules, and one draw needn't show every extreme that they name: Each row of lengths lays the responses of one micro-batch end to end over the 4096 positions.
All inputs are finite; a program needn't handle non-finite values.
Results may differ from the reference program's by a relative error of at most 0.0045.
Values may be sent and summed in bfloat16 or wider, within the bound.
A program may use at most 64 MiB of HBM per device.

```python
import math
import jax
import jax.numpy as jnp
import numpy as np
from jax import lax

D = 2048
HEAD_DIM = 64
HEADS = 16
KV_HEADS = 4
LAYERS = 16
TOKENS = 4096
QKV = 1536
RESP_MAX = 1024
DOCS = 8
N_PIPE = 16


def draw_states(key, part):
    entries = jnp.clip(jax.random.normal(jax.random.fold_in(key, 501), (LAYERS, TOKENS, D), jnp.float32), -6.0, 6.0)
    return entries.astype(jnp.bfloat16)


def draw_w_in(key, part):
    entries = jax.random.normal(jax.random.fold_in(key, 601), (LAYERS, D, QKV), jnp.float32) * D ** (-0.5)
    return jnp.clip(entries, -1.0, 1.0).astype(jnp.bfloat16)


def block_levels(stream_key, extent, pieces, low, top_value):
    factor_of = 1.0
    for dim, blocks in pieces:
        steps = jax.random.uniform(jax.random.fold_in(jax.random.fold_in(stream_key, 6), dim), (blocks,), jnp.float32, low / len(pieces), top_value / len(pieces))
        factor_of = factor_of * jnp.repeat(jnp.exp(steps), extent[dim] // blocks).reshape((-1,) + (1,) * (len(extent) - 1 - dim))
    return factor_of


def length_profile(amount, total, limit, skew):
    weights = [(1 << 20) // math.isqrt(standing ** skew) + 1 for standing in range(2, amount + 1)]
    rest, counts = total - limit - (amount - 1), [1] * (amount - 1)
    while rest > 0:
        movable = [i for i in range(amount - 1) if counts[i] < limit]
        pool, budget = sum([weights[i] for i in movable]), rest
        for i in movable:
            more = min(limit - counts[i], max(1, budget * weights[i] // pool), rest)
            counts[i] = counts[i] + more
            rest = rest - more
    return np.array([limit] + counts)


def ragged_sizes(own_key, count, total, most, skew):
    if count == 2:
        one = jax.random.randint(own_key, (), max(1, total - most), min(most, total - 1) + 1)
        return jnp.stack([one, total - one])
    tallies = jnp.asarray(length_profile(count, total, most, skew), jnp.int32)
    couples = (count - 1) // 2
    source_of, receiver = tallies[1:1 + 2 * couples:2], tallies[2:2 + 2 * couples:2]
    room = jnp.minimum(source_of - 1, most - receiver)
    passed = jax.random.randint(jax.random.fold_in(own_key, 1), (couples,), 0, 1 << 20) % (room + 1)
    tallies = tallies.at[1:1 + 2 * couples:2].set(source_of - passed).at[2:2 + 2 * couples:2].set(receiver + passed)
    return tallies[jax.random.permutation(jax.random.fold_in(own_key, 2), count)]


def noise(key, shape, deviation, limit, pieces=(), kind=jnp.bfloat16):
    level = block_levels(key, shape, pieces, -0.22, 0.18) if pieces else 1.0
    drawn = jax.random.normal(key, shape, jnp.float32) * deviation * level
    return jnp.minimum(jnp.maximum(drawn, -limit), limit).astype(kind)


def setup_inputs(seed: int = 0) -> dict:
    splits = jax.random.split(jax.random.key(seed), 6)
    states = draw_states(jax.random.fold_in(splits[5], 71), 0)
    norm_gain = jnp.clip(1.0 + 0.15 * jax.random.normal(splits[1], (LAYERS, D), jnp.float32), 0.25, 1.75)
    w_in = draw_w_in(jax.random.fold_in(splits[5], 71), 0)
    w_out = noise(splits[3], (LAYERS, HEADS * HEAD_DIM, D), (HEADS * HEAD_DIM) ** -0.5, 0.1875, ((0, 16), (1, 32)))
    lengths = jax.vmap(lambda own: ragged_sizes(own, DOCS, TOKENS, RESP_MAX, 1))(jax.random.split(splits[4], LAYERS)).reshape((LAYERS, DOCS)).astype(jnp.int32)
    return {"states": states, "norm_gain": norm_gain, "w_in": w_in, "w_out": w_out, "lengths": lengths}


epsilon = 1e-05
rope_base = 500000.0
masked_score = -1e+30

def locate(doc_lengths, spots):
    doc_ends = jnp.cumsum(doc_lengths).astype(jnp.int32)
    segment = lax.optimization_barrier(jnp.sum((doc_ends[None, :] <= spots[:, None]).astype(jnp.int32), axis=1)).astype(jnp.int32)
    starts = (doc_ends - doc_lengths).astype(jnp.int32)
    labels = jnp.arange(doc_lengths.shape[0], dtype=jnp.int32)
    first = lax.optimization_barrier(jnp.sum(jnp.where(segment[:, None] == labels[None, :], starts[None, :], 0), axis=1)).astype(jnp.int32)
    return (segment, (spots - first).astype(jnp.int32))

def rotate_pairs(heads_data, position):
    half_dim = heads_data.shape[-1] // 2
    inverse = rope_base ** (-jnp.arange(half_dim, dtype=jnp.float32) * 2.0 / heads_data.shape[-1])
    angles = position.astype(jnp.float32)[:, None] * inverse[None, :]
    cosine = jnp.cos(angles)[:, None, :]
    sine_part = jnp.sin(angles)[:, None, :]
    first_half = heads_data[..., :half_dim]
    second_half = heads_data[..., half_dim:]
    return jnp.concatenate([first_half * cosine - second_half * sine_part, second_half * cosine + first_half * sine_part], -1)

def attention_layer(inputs, gain, weight_in, weight_out, doc_lengths):
    wide = inputs.astype(jnp.float32)
    normed = (wide * lax.rsqrt(lax.optimization_barrier(jnp.mean(wide * wide, -1, keepdims=True)) + epsilon) * gain).astype(jnp.bfloat16)
    proj = jnp.dot(normed, weight_in, preferred_element_type=jnp.float32)
    q_width = HEADS * HEAD_DIM
    k_width = KV_HEADS * HEAD_DIM
    spots = jnp.arange(TOKENS, dtype=jnp.int32)
    segment, position = locate(doc_lengths, spots)
    queries = rotate_pairs(proj[:, :q_width].reshape(TOKENS, HEADS, HEAD_DIM), position).astype(jnp.bfloat16)
    keys_rot = rotate_pairs(proj[:, q_width:q_width + k_width].reshape(TOKENS, KV_HEADS, HEAD_DIM), position).astype(jnp.bfloat16)
    values = proj[:, q_width + k_width:].reshape(TOKENS, KV_HEADS, HEAD_DIM).astype(jnp.bfloat16)
    group = HEADS // KV_HEADS
    keys_wide = keys_rot.astype(jnp.float32)
    values_wide = values.astype(jnp.float32)
    block_rows = math.gcd(TOKENS, 512)

    def query_block(block_idx):
        first_row = block_idx * block_rows
        query_part = lax.dynamic_slice_in_dim(queries, first_row, block_rows, 0).astype(jnp.float32)
        query_part = query_part.reshape(block_rows, KV_HEADS, group, HEAD_DIM)
        scores = jnp.einsum('tgjd,rgd->gjtr', query_part, keys_wide) * HEAD_DIM ** (-0.5)
        query_spots = first_row + jnp.arange(block_rows, dtype=jnp.int32)
        query_seg = lax.dynamic_slice_in_dim(segment, first_row, block_rows, 0)
        allowed = (query_seg[:, None] == segment[None, :]) & (spots[None, :] <= query_spots[:, None])
        scores = jnp.where(allowed, scores, masked_score)
        row_max = lax.optimization_barrier(jnp.max(scores, -1, keepdims=True))
        probs = jnp.where(allowed, jnp.exp(scores - row_max), 0.0)
        denom = lax.optimization_barrier(jnp.sum(probs, -1))
        rounded = probs.astype(jnp.bfloat16).astype(jnp.float32)
        attended = jnp.einsum('gjtr,rgd->gjtd', rounded, values_wide) / denom[..., None]
        return attended.transpose(2, 0, 1, 3).reshape(block_rows, HEADS * HEAD_DIM).astype(jnp.bfloat16)
    attended = lax.map(query_block, jnp.arange(TOKENS // block_rows, dtype=jnp.int32))
    attended = attended.reshape(TOKENS, HEADS * HEAD_DIM)
    output = jnp.dot(attended, weight_out, preferred_element_type=jnp.float32)
    return (wide + output).astype(jnp.bfloat16)

def reference(states, norm_gain, w_in, w_out, lengths):
    results = []
    for section_index in range(N_PIPE):
        results.append(attention_layer(states[section_index], norm_gain[section_index], w_in[section_index], w_out[section_index], lengths[section_index]))
    return jnp.stack([results[(section_index - 1) % N_PIPE] for section_index in range(N_PIPE)])
```

```python
import functools
import math

import jax
import jax.numpy as jnp
from jax import lax
from jax.experimental import pallas as pl
from jax.experimental.pallas import tpu as pltpu
from jax.sharding import Mesh
from jax.sharding import PartitionSpec as P

HEAD_DIM = 64
HEADS = 16
KV_HEADS = 4
GROUP = HEADS // KV_HEADS
NX = 4
CHUNKS = 2
WINDOW = 9
COLS = (GROUP + 2) * HEAD_DIM

epsilon = 1e-05
rope_base = 500000.0
masked_score = -1e30
MESH = pl.DeviceIdType.MESH


def sine_cosine(angle):
    turns = jnp.floor(angle * (2.0 / math.pi) + 0.5)
    quarter = turns.astype(jnp.int32)
    rest = angle - turns * 1.5703125
    rest = rest - turns * 4.837512969970703125e-4
    rest = rest - turns * 7.54978995489188216e-8
    z = rest * rest
    sine = ((-1.9515295891e-4 * z + 8.3321608736e-3) * z - 1.6666654611e-1) * z * rest + rest
    cosine = (
        (2.443315711809948e-5 * z - 1.388731625493765e-3) * z + 4.166664568298827e-2
    ) * z * z - 0.5 * z + 1.0
    odd = (quarter & 1) == 1
    sine, cosine = jnp.where(odd, cosine, sine), jnp.where(odd, sine, cosine)
    sine = jnp.where((quarter & 2) == 2, -sine, sine)
    cosine = jnp.where(((quarter + 1) & 2) == 2, -cosine, cosine)
    return sine, cosine


def response_start(ends, spots):
    start = jnp.zeros_like(spots)
    for end in ends:
        start = jnp.maximum(start, jnp.where(spots >= end, end, 0))
    return start


def tick_kernel(
    n_pipe,
    n_y,
    lengths,
    inverse,
    gain,
    x_hbm,
    wi_hbm,
    wo_hbm,
    out,
    xg,
    xn,
    wloc,
    wsp,
    wi,
    wo,
    trig,
    q_s,
    kv,
    att,
    acc,
    obuf,
    local_sem,
    send_sem,
    recv_sem,
):
    p = lax.axis_index("pipe")
    y = lax.axis_index("ctx_y")
    x = lax.axis_index("ctx_x")
    rows = xg.shape[1]
    half = rows // 2
    part = rows // CHUNKS
    depth = xg.shape[2]
    out_cols = acc.shape[1]
    span = NX * rows

    def xs(d):
        return lax.rem(x + (d + NX), NX)

    def ys(d):
        return lax.rem(y + (d + n_y), n_y)

    def ps(d):
        return lax.rem(p + (d + n_pipe), n_pipe)

    counter = [0]
    pending = []

    def send(src, dst, device, landing=None):
        k = counter[0]
        counter[0] += 1
        copy = pltpu.make_async_remote_copy(
            src_ref=src,
            dst_ref=dst,
            send_sem=send_sem.at[k],
            recv_sem=recv_sem.at[k],
            device_id=device,
            device_id_type=MESH,
        )
        copy.start()
        pending.append(copy)
        land = dst if landing is None else landing

        def arrive():
            pltpu.make_async_remote_copy(
                src_ref=land,
                dst_ref=land,
                send_sem=send_sem.at[k],
                recv_sem=recv_sem.at[k],
                device_id=device,
                device_id_type=MESH,
            ).wait_recv()

        return arrive

    load_w = pltpu.make_async_copy(wi_hbm, wloc, local_sem.at[0])
    load_x = pltpu.make_async_copy(x_hbm, xg.at[0], local_sem.at[1])
    own_cols = pl.ds(pl.multiple_of(x * out_cols, out_cols), out_cols)
    load_o = pltpu.make_async_copy(
        wo_hbm.at[:, own_cols], wo.at[y, x // 2, lax.rem(x, 2)], local_sem.at[2]
    )
    load_w.start()
    load_x.start()
    load_o.start()

    barrier = pltpu.get_barrier_semaphore()
    peers = [(p, y, xs(d)) for d in (1, 2, 3)]
    peers += [(p, ys(d), x) for d in (1, -1)]
    peers += [(ps(e), y, xs(d)) for e in (1, -1) for d in range(NX)]
    for peer in peers:
        pl.semaphore_signal(barrier, inc=1, device_id=peer, device_id_type=MESH)

    load_w.wait()
    w_rows = wloc.shape[0]
    lane_w = lax.broadcasted_iota(jnp.int32, (w_rows, 128), 1)
    q_width = HEADS * HEAD_DIM
    g_width = GROUP * HEAD_DIM
    for t in range(NX):
        k_tile = wloc[:, q_width + 128 * (t // 2) : q_width + 128 * (t // 2) + 128]
        v_at = q_width + KV_HEADS * HEAD_DIM + 128 * (t // 2)
        v_tile = wloc[:, v_at : v_at + 128]
        k_tile = k_tile.astype(jnp.float32)
        v_tile = v_tile.astype(jnp.float32)
        if t % 2 == 0:
            v_tile = pltpu.roll(v_tile, 64, 1)
        else:
            k_tile = pltpu.roll(k_tile, 64, 1)
        wsp[t, :, :g_width] = wloc[:, g_width * t : g_width * (t + 1)]
        wsp[t, :, g_width:] = jnp.where(lane_w < 64, k_tile, v_tile).astype(jnp.bfloat16)
    wi[y, x // 2, lax.rem(x, 2)] = wsp[x]
    load_x.wait()
    pl.semaphore_wait(barrier, len(peers))

    def place(buf, yy, xx):
        return buf.at[yy, xx // 2, lax.rem(xx, 2)]

    wi_in = [
        send(wsp.at[xs(d)], place(wi, y, x), (p, y, xs(d)), place(wi, y, xs(-d)))
        for d in (1, -1, 2)
    ]
    first, second = pl.ds(0, half), pl.ds(half, half)
    up, down = (p, y, xs(1)), (p, y, xs(-1))
    x_up_a = send(xg.at[0, first], xg.at[1, first], up)
    x_down_b = send(xg.at[0, second], xg.at[2, second], down)
    x_up_b = send(xg.at[0, second], xg.at[1, second], up)
    x_down_a = send(xg.at[0, first], xg.at[2, first], down)

    north, south = (p, ys(1), x), (p, ys(-1), x)
    reach = n_y // 2

    def ring_send(buf, step):
        arrivals = []
        order = ((0, 1), (1, -1), (1, 1), (0, -1))
        for u, way in order:
            if step == reach - 1 and (u, way) not in ((0, 1), (1, -1)):
                continue
            piece = buf.at[ys(-way * step), u]
            landing = buf.at[ys(-way * (step + 1)), u]
            arrivals.append((u, way, piece, landing))
        return arrivals

    def ring_start(buf):
        return [
            send(piece, piece, north if way == 1 else south, landing)
            for u, way, piece, landing in ring_send(buf, 0)
        ]

    def ring_step(buf, step, arrivals):
        following = {(u, way): (piece, landing) for u, way, piece, landing in (
            ring_send(buf, step + 1) if step + 1 < reach else []
        )}
        result = []
        for (u, way, _, _), arrive in zip(ring_send(buf, step), arrivals):
            arrive()
            if (u, way) in following:
                piece, landing = following[(u, way)]
                result.append(send(piece, piece, north if way == 1 else south, landing))
        return result

    for arrive in wi_in:
        arrive()
    wi_ring = ring_start(wi)

    ends = []
    total = 0
    for i in range(lengths.shape[1]):
        total = total + lengths[p, i]
        ends.append(total)
    deltas = (0, -1, 1, 2)
    lane = lax.broadcasted_iota(jnp.int32, (rows, 128), 1)
    row = lax.broadcasted_iota(jnp.int32, (rows, 128), 0)

    def make_trig(slot):
        spots = y * span + xs(deltas[slot]) * rows + row
        place_in = (spots - response_start(ends, spots)).astype(jnp.float32)
        sine, cosine = sine_cosine(place_in * inverse[...])
        trig[slot, 0] = cosine
        trig[slot, 1] = jnp.where((lane & 63) < 32, -sine, sine)

    norm_rows = 16

    def normalize(slot):
        def step(i, carry):
            at = pl.ds(pl.multiple_of(i * norm_rows, norm_rows), norm_rows)
            wide = xg[slot, at, :].astype(jnp.float32)
            scale = lax.rsqrt(jnp.mean(wide * wide, -1, keepdims=True) + epsilon)
            to = pl.ds(pl.multiple_of(slot * rows + i * norm_rows, norm_rows), norm_rows)
            xn[to, :] = (wide * scale * gain[...]).astype(jnp.bfloat16)
            return carry

        lax.fori_loop(0, rows // norm_rows, step, 0)

    for slot in range(4):
        make_trig(slot)
    normalize(0)

    wi_ring = ring_step(wi, 0, wi_ring)
    x_up_a()
    x_far_a = send(xg.at[1, first], xg.at[3, first], up)
    x_down_b()
    x_far_b = send(xg.at[2, second], xg.at[3, second], down)
    wo_in = []
    for d in (1, -1, 2):
        cols = pl.ds(pl.multiple_of(xs(d) * out_cols, out_cols), out_cols)
        wo_in.append(
            send(wo_hbm.at[:, cols], place(wo, y, x), (p, y, xs(d)), place(wo, y, xs(-d)))
        )
    for step in range(1, reach - 1):
        wi_ring = ring_step(wi, step, wi_ring)
    x_up_b()
    normalize(1)
    x_down_a()
    normalize(2)
    load_o.wait()
    for arrive in wo_in:
        arrive()
    wo_ring = ring_start(wo)
    wi_ring = ring_step(wi, reach - 1, wi_ring)

    def project(slot, count):
        proj = jnp.dot(
            xn[slot * rows : (slot + count) * rows, :],
            wi[...].reshape(depth, COLS),
            preferred_element_type=jnp.float32,
        )
        arrivals = []
        for i in range(count):
            own = proj[i * rows : (i + 1) * rows]
            cosine, sine = trig[slot + i, 0], trig[slot + i, 1]
            block = xs(deltas[slot + i])

            def rotated(tile):
                partner = jnp.where(
                    (lane & 63) < 32, pltpu.roll(tile, 96, 1), pltpu.roll(tile, 32, 1)
                )
                return tile * cosine + partner * sine

            tail = own[:, g_width:]
            kv[2 * NX + block] = jnp.where(lane < 64, rotated(tail), tail).astype(jnp.bfloat16)
            arrivals.append(
                send(kv.at[2 * NX + block], kv.at[NX + block], north)
            )
            for t in range(GROUP // 2):
                tile = rotated(own[:, 128 * t : 128 * (t + 1)]) * HEAD_DIM**-0.5
                q_s[block, 2 * t] = jnp.where(lane < 64, tile, 0.0).astype(jnp.bfloat16)
                q_s[block, 2 * t + 1] = jnp.where(
                    lane < 64, pltpu.roll(tile, 64, 1), 0.0
                ).astype(jnp.bfloat16)
        return arrivals

    near = project(0, 3)
    x_far_a()
    x_far_b()
    normalize(3)
    near += project(3, 1)
    wo_ring = ring_step(wo, 0, wo_ring)
    far = []
    for slot in range(4):
        near[slot]()
        block = xs(deltas[slot])
        far.append(send(kv.at[NX + block], kv.at[block], north))
    for step in range(1, reach - 1):
        wo_ring = ring_step(wo, step, wo_ring)
    for arrive in far:
        arrive()

    lane_p = lax.broadcasted_iota(jnp.int32, (part, 128), 1)
    row_p = lax.broadcasted_iota(jnp.int32, (part, 128), 0)

    def attend(i):
        def one(j, carry):
            queries = q_s[j, :, i * part : (i + 1) * part, :].reshape(GROUP * part, 128)
            window = kv[pl.ds(j, WINDOW)].reshape(WINDOW * rows, 128)
            scores = lax.dot_general(
                queries, window, (((1,), (1,)), ((), ())), preferred_element_type=jnp.float32
            )
            spots = y * span + j * rows + i * part + row_p
            start = response_start(ends, spots)
            allowed = []
            for c in range(WINDOW):
                keys = y * span + (j + c - 2 * NX) * rows + lane_p
                allowed.append((keys >= start) & (keys <= spots))
            allowed = jnp.concatenate(allowed, 1)
            scores = jnp.where(
                allowed[None], scores.reshape(GROUP, part, WINDOW * rows), masked_score
            )
            probs = jnp.exp(scores - jnp.max(scores, -1, keepdims=True))
            denom = jnp.sum(probs, -1, keepdims=True)
            mixed = jnp.dot(
                probs.astype(jnp.bfloat16).reshape(GROUP * part, WINDOW * rows),
                window,
                preferred_element_type=jnp.float32,
            ).reshape(GROUP, part, 128)
            mixed = mixed / denom
            tiles = [
                jnp.where(lane_p < 64, pltpu.roll(mixed[2 * t], 64, 1), mixed[2 * t + 1])
                for t in range(GROUP // 2)
            ]
            att[i, x, j] = jnp.concatenate(tiles, 1).astype(jnp.bfloat16)
            return carry

        lax.fori_loop(0, NX, one, 0)

    low, high = pl.ds(0, NX // 2), pl.ds(NX // 2, NX // 2)

    def att_start(i):
        return (
            send(att.at[i, x, low], att.at[i, x, low], up, att.at[i, xs(-1), low]),
            send(att.at[i, x, high], att.at[i, x, high], down, att.at[i, xs(1), high]),
            send(att.at[i, x, high], att.at[i, x, high], up, att.at[i, xs(-1), high]),
            send(att.at[i, x, low], att.at[i, x, low], down, att.at[i, xs(1), low]),
        )

    def att_pass(i, arrivals):
        arrivals[0]()
        piece = att.at[i, xs(-1), low]
        far_low = send(piece, piece, up, att.at[i, xs(2), low])
        arrivals[1]()
        piece = att.at[i, xs(1), high]
        far_high = send(piece, piece, down, att.at[i, xs(2), high])
        return (arrivals[2], arrivals[3], far_low, far_high)

    def finish(i):
        weight = wo[...].reshape(q_width, out_cols)
        result = None
        for h in range(NX):
            term = jnp.dot(
                att[i, h].reshape(NX * part, g_width),
                weight[h * g_width : (h + 1) * g_width],
                preferred_element_type=jnp.float32,
            )
            result = term if result is None else result + term
        acc[...] = result
        arrivals = []
        for slot in (3, 2, 1, 0):
            d = deltas[slot]
            j = xs(d)
            kept = xg[slot, i * part : (i + 1) * part, own_cols].astype(jnp.float32)
            at = pl.ds(pl.multiple_of(j * part, part), part)
            obuf[i, slot] = (acc[at, :] + kept).astype(jnp.bfloat16)
            from_cols = pl.ds(pl.multiple_of(xs(-d) * out_cols, out_cols), out_cols)
            there = pl.ds(i * part, part)
            arrivals.append(
                send(
                    obuf.at[i, slot],
                    out.at[there, own_cols],
                    (ps(1), y, j),
                    out.at[there, from_cols],
                )
            )
        return arrivals

    attend(0)
    arrivals_0 = att_start(0)
    wo_ring = ring_step(wo, reach - 1, wo_ring)
    attend(1)
    arrivals_1 = att_start(1)
    arrivals_0 = att_pass(0, arrivals_0)
    for arrive in arrivals_0:
        arrive()
    last = finish(0)
    for arrive in att_pass(1, arrivals_1):
        arrive()
    last += finish(1)
    for arrive in last:
        arrive()
    for copy in pending:
        copy.wait_send()


def body(states, norm_gain, w_in, w_out, lengths):
    rows, depth = states.shape[1:]
    w_rows = w_in.shape[1]
    o_rows = w_out.shape[1]
    out_cols = depth // NX
    n_pipe = lax.axis_size("pipe")
    n_y = lax.axis_size("ctx_y")
    part = rows // CHUNKS
    copies = 128
    half_dim = HEAD_DIM // 2
    inverse = rope_base ** (-jnp.arange(half_dim, dtype=jnp.float32) * 2.0 / HEAD_DIM)
    inverse = jnp.tile(inverse, 128 // half_dim)[None, :]
    bf16, f32 = jnp.bfloat16, jnp.float32
    moved = pl.pallas_call(
        functools.partial(tick_kernel, n_pipe, n_y),
        out_shape=jax.ShapeDtypeStruct((rows, depth), bf16),
        in_specs=[
            pl.BlockSpec(memory_space=pltpu.SMEM),
            pl.BlockSpec(memory_space=pltpu.VMEM),
            pl.BlockSpec(memory_space=pltpu.VMEM),
            pl.BlockSpec(memory_space=pl.ANY),
            pl.BlockSpec(memory_space=pl.ANY),
            pl.BlockSpec(memory_space=pl.ANY),
        ],
        out_specs=pl.BlockSpec(memory_space=pl.ANY),
        scratch_shapes=[
            pltpu.VMEM((4, rows, depth), bf16),
            pltpu.VMEM((4 * rows, depth), bf16),
            pltpu.VMEM((w_rows, w_in.shape[2]), bf16),
            pltpu.VMEM((NX, w_rows, COLS), bf16),
            pltpu.VMEM((n_y, 2, 2, w_rows, COLS), bf16),
            pltpu.VMEM((n_y, 2, 2, o_rows, out_cols), bf16),
            pltpu.VMEM((4, 2, rows, 128), f32),
            pltpu.VMEM((NX, GROUP, rows, 128), bf16),
            pltpu.VMEM((3 * NX, rows, 128), bf16),
            pltpu.VMEM((CHUNKS, NX, NX, part, GROUP * HEAD_DIM), bf16),
            pltpu.VMEM((NX * part, out_cols), f32),
            pltpu.VMEM((CHUNKS, 4, part, out_cols), bf16),
            pltpu.SemaphoreType.DMA((3,)),
            pltpu.SemaphoreType.DMA((copies,)),
            pltpu.SemaphoreType.DMA((copies,)),
        ],
        compiler_params=pltpu.CompilerParams(
            collective_id=0, has_side_effects=True, vmem_limit_bytes=60 * 1024 * 1024
        ),
        name="tick",
    )(lengths, inverse, norm_gain, states[0], w_in[0], w_out[0])
    return moved[None]


def solution(mesh):
    n_pipe = mesh.shape["pipe"]
    n_y = mesh.shape["ctx"] // NX
    finer = Mesh(mesh.devices.reshape(n_pipe, n_y, NX), ("pipe", "ctx_y", "ctx_x"))
    ctx = ("ctx_y", "ctx_x")
    placed = (
        P("pipe", ctx, None),
        P("pipe", None),
        P("pipe", ctx, None),
        P("pipe", ctx, None),
        P(),
    )
    return jax.shard_map(
        body, mesh=finer, in_specs=placed, out_specs=P("pipe", ctx, None), check_vma=False
    )
```

```python
import functools
import math

import jax
import jax.numpy as jnp
from jax import lax
from jax.experimental import pallas as pl
from jax.experimental.pallas import tpu as pltpu
from jax.sharding import Mesh
from jax.sharding import PartitionSpec as P

HEAD_DIM = 64
HEADS = 16
KV_HEADS = 4
GROUP = HEADS // KV_HEADS
NX = 4
CHUNKS = 2
WINDOW = 9
COLS = (GROUP + 2) * HEAD_DIM

epsilon = 1e-05
rope_base = 500000.0
masked_score = -1e30
MESH = pl.DeviceIdType.MESH


def sine_cosine(angle):
    turns = jnp.floor(angle * (2.0 / math.pi) + 0.5)
    quarter = turns.astype(jnp.int32)
    rest = angle - turns * 1.5703125
    rest = rest - turns * 4.837512969970703125e-4
    rest = rest - turns * 7.54978995489188216e-8
    z = rest * rest
    sine = ((-1.9515295891e-4 * z + 8.3321608736e-3) * z - 1.6666654611e-1) * z * rest + rest
    cosine = (
        (2.443315711809948e-5 * z - 1.388731625493765e-3) * z + 4.166664568298827e-2
    ) * z * z - 0.5 * z + 1.0
    odd = (quarter & 1) == 1
    sine, cosine = jnp.where(odd, cosine, sine), jnp.where(odd, sine, cosine)
    sine = jnp.where((quarter & 2) == 2, -sine, sine)
    cosine = jnp.where(((quarter + 1) & 2) == 2, -cosine, cosine)
    return sine, cosine


def response_start(ends, spots):
    start = jnp.zeros_like(spots)
    for end in ends:
        start = jnp.maximum(start, jnp.where(spots >= end, end, 0))
    return start


def tick_kernel(
    n_pipe,
    n_y,
    lengths_hbm,
    gain_hbm,
    x_hbm,
    wi_hbm,
    wo_hbm,
    out,
    lengths,
    gain,
    xg,
    xn,
    wloc,
    wsp,
    wi,
    wo,
    trig,
    q_s,
    kv,
    v_one,
    att,
    acc,
    obuf,
    local_sem,
    send_sem,
    recv_sem,
):
    p = lax.axis_index("pipe")
    y = lax.axis_index("ctx_y")
    x = lax.axis_index("ctx_x")
    rows = xg.shape[1]
    half = rows // 2
    part = rows // CHUNKS
    depth = xg.shape[2]
    out_cols = acc.shape[1]
    span = NX * rows

    def xs(d):
        return lax.rem(x + (d + NX), NX)

    def ys(d):
        return lax.rem(y + (d + n_y), n_y)

    def ps(d):
        return lax.rem(p + (d + n_pipe), n_pipe)

    counter = [0]
    pending = []

    def send(src, dst, device, landing=None):
        k = counter[0]
        counter[0] += 1
        copy = pltpu.make_async_remote_copy(
            src_ref=src,
            dst_ref=dst,
            send_sem=send_sem.at[k],
            recv_sem=recv_sem.at[k],
            device_id=device,
            device_id_type=MESH,
        )
        copy.start()
        pending.append(copy)
        land = dst if landing is None else landing

        def arrive():
            pltpu.make_async_remote_copy(
                src_ref=land,
                dst_ref=land,
                send_sem=send_sem.at[k],
                recv_sem=recv_sem.at[k],
                device_id=device,
                device_id_type=MESH,
            ).wait_recv()

        return arrive

    load_w = pltpu.make_async_copy(wi_hbm, wloc, local_sem.at[0])
    load_x = pltpu.make_async_copy(x_hbm, xg.at[0], local_sem.at[1])
    own_cols = pl.ds(pl.multiple_of(x * out_cols, out_cols), out_cols)
    load_o = pltpu.make_async_copy(
        wo_hbm.at[:, own_cols], wo.at[y, x // 2, lax.rem(x, 2)], local_sem.at[2]
    )
    load_g = pltpu.make_async_copy(gain_hbm, gain, local_sem.at[3])
    load_l = pltpu.make_async_copy(lengths_hbm, lengths, local_sem.at[4])
    load_w.start()
    load_x.start()

    barrier = pltpu.get_barrier_semaphore()
    peers = [(p, y, xs(d)) for d in (1, 2, 3)]
    peers += [(p, ys(d), x) for d in (1, -1)]
    peers += [(ps(e), y, xs(d)) for e in (1, -1) for d in range(NX)]
    for peer in peers:
        pl.semaphore_signal(barrier, inc=1, device_id=peer, device_id_type=MESH)
    load_l.start()
    load_g.start()
    load_o.start()

    load_w.wait()
    w_rows = wloc.shape[0]
    lane_w = lax.broadcasted_iota(jnp.int32, (w_rows, 128), 1)
    q_width = HEADS * HEAD_DIM
    g_width = GROUP * HEAD_DIM
    for t in range(NX):
        k_tile = wloc[:, q_width + 128 * (t // 2) : q_width + 128 * (t // 2) + 128]
        v_at = q_width + KV_HEADS * HEAD_DIM + 128 * (t // 2)
        v_tile = wloc[:, v_at : v_at + 128]
        k_tile = k_tile.astype(jnp.float32)
        v_tile = v_tile.astype(jnp.float32)
        if t % 2 == 0:
            v_tile = pltpu.roll(v_tile, 64, 1)
        else:
            k_tile = pltpu.roll(k_tile, 64, 1)
        wsp[t, :, :g_width] = wloc[:, g_width * t : g_width * (t + 1)]
        wsp[t, :, g_width:] = jnp.where(lane_w < 64, k_tile, v_tile).astype(jnp.bfloat16)
    wi[y, x] = wsp[x]
    load_x.wait()
    with jax.named_scope("barrier"):
        pl.semaphore_wait(barrier, len(peers))

    def place(buf, yy, xx):
        return buf.at[yy, xx // 2, lax.rem(xx, 2)]

    north, south = (p, ys(1), x), (p, ys(-1), x)
    toward = {1: north, -1: south}
    reach = n_y // 2

    def piece_wi(dy, d):
        return wi.at[ys(dy), xs(d)]

    def piece_wo(dy, u):
        return wo.at[ys(dy), u]

    wi_order = ((0, 1), (0, -1), (-1, 1), (1, -1), (1, 1), (-1, -1), (2, 1), (2, -1))
    wi_final = ((0, 1), (1, -1), (-1, 1), (2, -1))
    wo_order = ((0, 1), (1, -1), (1, 1), (0, -1))
    wo_final = ((0, 1), (1, -1))

    def ring_send(piece, u, way, step):
        source = piece(-way * step, u)
        return send(source, source, toward[way], piece(-way * (step + 1), u))

    def ring_step(piece, order, final, step, arrivals):
        result = {}
        for key in order:
            if key not in arrivals:
                continue
            arrivals[key]()
            if step + 1 < reach - 1 or (step + 1 == reach - 1 and key in final):
                result[key] = ring_send(piece, key[0], key[1], step + 1)
        return result

    wi_ring = {(0, way): ring_send(piece_wi, 0, way, 0) for way in (1, -1)}
    wi_in = {
        -d: send(wsp.at[xs(d)], piece_wi(0, 0), (p, y, xs(d)), piece_wi(0, -d))
        for d in (1, -1)
    }
    wi_in[2] = send(wsp.at[xs(2)], piece_wi(0, 0), (p, y, xs(2)), piece_wi(0, 2))
    first, second = pl.ds(0, half), pl.ds(half, half)
    up, down = (p, y, xs(1)), (p, y, xs(-1))
    x_up_a = send(xg.at[0, first], xg.at[1, first], up)
    x_down_b = send(xg.at[0, second], xg.at[2, second], down)
    x_up_b = send(xg.at[0, second], xg.at[1, second], up)
    x_down_a = send(xg.at[0, first], xg.at[2, first], down)
    for d in (-1, 1, 2):
        with jax.named_scope(f"wi_in{d}"):
            wi_in[d]()
        for way in (1, -1):
            wi_ring[d, way] = ring_send(piece_wi, d, way, 0)

    load_l.wait()
    load_g.wait()
    ends = []
    total = 0
    for i in range(lengths.shape[0]):
        total = total + lengths[i, p]
        ends.append(total)
    deltas = (0, -1, 1, 2)
    lane = lax.broadcasted_iota(jnp.int32, (rows, 128), 1)
    row = lax.broadcasted_iota(jnp.int32, (rows, 128), 0)
    half_dim = HEAD_DIM // 2
    turn = lax.broadcasted_iota(jnp.int32, (8, 128), 1) & (half_dim - 1)
    inverse = jnp.zeros((8, 128), jnp.float32)
    for i in range(half_dim):
        inverse = jnp.where(turn == i, rope_base ** (-2.0 * i / HEAD_DIM), inverse)

    def make_trig(slot):
        spots = y * span + xs(deltas[slot]) * rows + row
        place_in = (spots - response_start(ends, spots)).astype(jnp.float32)
        sine, cosine = sine_cosine(place_in * inverse[:1])
        trig[slot, 0] = cosine
        trig[slot, 1] = jnp.where((lane & 63) < 32, -sine, sine)

    norm_rows = 32

    def normalize(slot):
        def step(i, carry):
            at = pl.ds(pl.multiple_of(i * norm_rows, norm_rows), norm_rows)
            wide = xg[slot, at, :].astype(jnp.float32)
            scale = lax.rsqrt(jnp.mean(wide * wide, -1, keepdims=True) + epsilon)
            to = pl.ds(pl.multiple_of(slot * rows + i * norm_rows, norm_rows), norm_rows)
            xn[to, :] = (wide * scale * gain[...]).astype(jnp.bfloat16)
            return carry

        lax.fori_loop(0, rows // norm_rows, step, 0, unroll=2)

    with jax.named_scope("trig"):
        for slot in range(4):
            make_trig(slot)
    with jax.named_scope("norm0"):
        normalize(0)

    with jax.named_scope("ring0"):
        wi_ring = ring_step(piece_wi, wi_order, wi_final, 0, wi_ring)
    with jax.named_scope("x_first"):
        x_up_a()
        x_far_a = send(xg.at[1, first], xg.at[3, first], up)
        x_down_b()
        x_far_b = send(xg.at[2, second], xg.at[3, second], down)
    wo_in = []
    for d in (1, -1, 2):
        cols = pl.ds(pl.multiple_of(xs(d) * out_cols, out_cols), out_cols)
        wo_in.append(
            send(wo_hbm.at[:, cols], place(wo, y, x), (p, y, xs(d)), place(wo, y, xs(-d)))
        )
    with jax.named_scope("ring12"):
        for step in range(1, reach - 1):
            wi_ring = ring_step(piece_wi, wi_order, wi_final, step, wi_ring)
    with jax.named_scope("x_second"):
        x_up_b()
        x_down_a()
    with jax.named_scope("norm12"):
        normalize(1)
        normalize(2)
    with jax.named_scope("ring3"):
        wi_ring = ring_step(piece_wi, wi_order, wi_final, reach - 1, wi_ring)

    def rotated(tile, slot):
        partner = jnp.where((lane & 63) < 32, pltpu.roll(tile, 96, 1), pltpu.roll(tile, 32, 1))
        return tile * trig[slot, 0] + partner * trig[slot, 1]

    def project(slot, count, first_col, last_col):
        return jnp.dot(
            xn[slot * rows : (slot + count) * rows, :],
            wi[:, :, :, first_col:last_col].reshape(depth, last_col - first_col),
            preferred_element_type=jnp.float32,
        )

    def project_kv(slot, count):
        proj = project(slot, count, g_width, COLS)
        arrivals = []
        for i in range(count):
            own = proj[i * rows : (i + 1) * rows]
            block = xs(deltas[slot + i])
            own = jnp.where(lane < 64, rotated(own, slot + i), own)
            kv[2 * NX + block] = own.astype(jnp.bfloat16)
            arrivals.append(send(kv.at[2 * NX + block], kv.at[NX + block], north))
        return arrivals

    def project_q(slot, count):
        proj = project(slot, count, 0, g_width)
        for i in range(count):
            own = proj[i * rows : (i + 1) * rows]
            block = xs(deltas[slot + i])
            for t in range(GROUP // 2):
                tile = rotated(own[:, 128 * t : 128 * (t + 1)], slot + i) * HEAD_DIM**-0.5
                q_s[block, 2 * t] = jnp.where(lane < 64, tile, 0.0).astype(jnp.bfloat16)
                q_s[block, 2 * t + 1] = jnp.where(
                    lane < 64, pltpu.roll(tile, 64, 1), 0.0
                ).astype(jnp.bfloat16)

    with jax.named_scope("kv012"):
        near = project_kv(0, 3)
    with jax.named_scope("x_far"):
        x_far_a()
        x_far_b()
    with jax.named_scope("norm3"):
        normalize(3)
    with jax.named_scope("kv3"):
        near += project_kv(3, 1)
    block = xs(deltas[3])
    far = [send(kv.at[2 * NX + block], kv.at[block], (p, ys(2), x))]
    with jax.named_scope("wo_in"):
        load_o.wait()
        for arrive in wo_in:
            arrive()
    wo_ring = {key: ring_send(piece_wo, *key, 0) for key in wo_order if key[1] == -1}
    with jax.named_scope("q012"):
        project_q(0, 3)
    with jax.named_scope("kv_near"):
        for slot in range(3):
            near[slot]()
            block = xs(deltas[slot])
            far.append(send(kv.at[NX + block], kv.at[block], north))
    wo_ring.update({key: ring_send(piece_wo, *key, 0) for key in wo_order if key[1] == 1})
    with jax.named_scope("q3"):
        project_q(3, 1)
    with jax.named_scope("kv_far"):
        near[3]()
        for arrive in far:
            arrive()
    with jax.named_scope("v_one"):
        for b in range(3 * NX):
            v_one[b] = jnp.where(lane < 64, 1.0, kv[b].astype(jnp.float32)).astype(jnp.bfloat16)

    lane_p = lax.broadcasted_iota(jnp.int32, (part, 128), 1)
    row_p = lax.broadcasted_iota(jnp.int32, (part, 128), 0)

    def attend(i, j):
        queries = q_s[j, :, i * part : (i + 1) * part, :].reshape(GROUP * part, 128)
        window = kv[j : j + WINDOW].reshape(WINDOW * rows, 128)
        values = v_one[j : j + WINDOW].reshape(WINDOW * rows, 128)
        scores = lax.dot_general(
            queries, window, (((1,), (1,)), ((), ())), preferred_element_type=jnp.float32
        )
        spots = y * span + j * rows + i * part + row_p
        start = response_start(ends, spots)
        allowed = []
        for c in range(WINDOW):
            keys = y * span + (j + c - 2 * NX) * rows + lane_p
            inside = keys >= start
            if c == WINDOW - 1:
                inside = inside & (keys <= spots)
            allowed.append(inside)
        allowed = jnp.concatenate(allowed, 1)
        scores = jnp.where(
            allowed[None], scores.reshape(GROUP, part, WINDOW * rows), masked_score
        )
        probs = jnp.exp(scores - jnp.max(scores, -1, keepdims=True))
        mixed = jnp.dot(
            probs.astype(jnp.bfloat16).reshape(GROUP * part, WINDOW * rows),
            values,
            preferred_element_type=jnp.float32,
        )
        turned = pltpu.roll(mixed, 64, 1)
        tiles = []
        for t in range(GROUP // 2):
            even = slice(2 * t * part, (2 * t + 1) * part)
            odd = slice((2 * t + 1) * part, (2 * t + 2) * part)
            tiles.append(
                jnp.where(lane_p < 64, turned[even] / mixed[even], mixed[odd] / turned[odd])
            )
        att[i, x, j] = jnp.concatenate(tiles, 1).astype(jnp.bfloat16)

    low, high = pl.ds(0, NX // 2), pl.ds(NX // 2, NX // 2)

    def att_start(i):
        return (
            send(att.at[i, x, low], att.at[i, x, low], up, att.at[i, xs(-1), low]),
            send(att.at[i, x, high], att.at[i, x, high], down, att.at[i, xs(1), high]),
            send(att.at[i, x, high], att.at[i, x, high], up, att.at[i, xs(-1), high]),
            send(att.at[i, x, low], att.at[i, x, low], down, att.at[i, xs(1), low]),
        )

    def att_pass(i, arrivals):
        arrivals[0]()
        piece = att.at[i, xs(-1), low]
        far_low = send(piece, piece, up, att.at[i, xs(2), low])
        arrivals[1]()
        piece = att.at[i, xs(1), high]
        far_high = send(piece, piece, down, att.at[i, xs(2), high])
        return (arrivals[2], arrivals[3], far_low, far_high)

    def finish(i):
        weight = wo[...].reshape(q_width, out_cols)
        result = None
        for h in range(NX):
            term = jnp.dot(
                att[i, h].reshape(NX * part, g_width),
                weight[h * g_width : (h + 1) * g_width],
                preferred_element_type=jnp.float32,
            )
            result = term if result is None else result + term
        acc[...] = result
        arrivals = []
        for slot in (3, 2, 1, 0):
            d = deltas[slot]
            j = xs(d)
            kept = xg[slot, i * part : (i + 1) * part, own_cols].astype(jnp.float32)
            at = pl.ds(pl.multiple_of(j * part, part), part)
            obuf[i, slot] = (acc[at, :] + kept).astype(jnp.bfloat16)
            from_cols = pl.ds(pl.multiple_of(xs(-d) * out_cols, out_cols), out_cols)
            there = pl.ds(i * part, part)
            arrivals.append(
                send(
                    obuf.at[i, slot],
                    out.at[there, own_cols],
                    (ps(1), y, j),
                    out.at[there, from_cols],
                )
            )
        return arrivals

    with jax.named_scope("attend0a"):
        attend(0, 0)
        attend(0, 1)
    with jax.named_scope("wo0"):
        wo_ring = ring_step(piece_wo, wo_order, wo_final, 0, wo_ring)
    with jax.named_scope("attend0b"):
        attend(0, 2)
        attend(0, 3)
    arrivals_0 = att_start(0)
    with jax.named_scope("attend1a"):
        attend(1, 0)
        attend(1, 1)
    for step in range(1, reach - 2):
        with jax.named_scope("wo1"):
            wo_ring = ring_step(piece_wo, wo_order, wo_final, step, wo_ring)
    with jax.named_scope("attend1b"):
        attend(1, 2)
        attend(1, 3)
    with jax.named_scope("pass0"):
        arrivals_0 = att_pass(0, arrivals_0)
    arrivals_1 = att_start(1)
    with jax.named_scope("wo2"):
        if reach > 2:
            wo_ring = ring_step(piece_wo, wo_order, wo_final, reach - 2, wo_ring)
    with jax.named_scope("att0_in"):
        for arrive in arrivals_0:
            arrive()
    with jax.named_scope("pass1"):
        arrivals_1 = att_pass(1, arrivals_1)
    with jax.named_scope("wo3"):
        wo_ring = ring_step(piece_wo, wo_order, wo_final, reach - 1, wo_ring)
    with jax.named_scope("finish0"):
        last = finish(0)
    with jax.named_scope("att1_in"):
        for arrive in arrivals_1:
            arrive()
    with jax.named_scope("finish1"):
        last += finish(1)
    with jax.named_scope("out_in"):
        for arrive in last:
            arrive()
    with jax.named_scope("wait_send"):
        for copy in pending:
            copy.wait_send()


def body(states, norm_gain, w_in, w_out, lengths):
    rows, depth = states.shape[1:]
    w_rows = w_in.shape[1]
    o_rows = w_out.shape[1]
    out_cols = depth // NX
    n_pipe = lax.axis_size("pipe")
    n_y = lax.axis_size("ctx_y")
    part = rows // CHUNKS
    copies = 128
    bf16, f32 = jnp.bfloat16, jnp.float32
    moved = pl.pallas_call(
        functools.partial(tick_kernel, n_pipe, n_y),
        out_shape=pltpu.VMEM((rows, depth), bf16),
        in_specs=[
            pl.BlockSpec(memory_space=pl.ANY),
            pl.BlockSpec(memory_space=pl.ANY),
            pl.BlockSpec(memory_space=pl.ANY),
            pl.BlockSpec(memory_space=pl.ANY),
            pl.BlockSpec(memory_space=pl.ANY),
        ],
        out_specs=pl.BlockSpec(memory_space=pltpu.VMEM),
        scratch_shapes=[
            pltpu.SMEM(lengths.shape[::-1], jnp.int32),
            pltpu.VMEM((1, depth), f32),
            pltpu.VMEM((4, rows, depth), bf16),
            pltpu.VMEM((4 * rows, depth), bf16),
            pltpu.VMEM((w_rows, w_in.shape[2]), bf16),
            pltpu.VMEM((NX, w_rows, COLS), bf16),
            pltpu.VMEM((n_y, NX, w_rows, COLS), bf16),
            pltpu.VMEM((n_y, 2, 2, o_rows, out_cols), bf16),
            pltpu.VMEM((4, 2, rows, 128), f32),
            pltpu.VMEM((NX, GROUP, rows, 128), bf16),
            pltpu.VMEM((3 * NX, rows, 128), bf16),
            pltpu.VMEM((3 * NX, rows, 128), bf16),
            pltpu.VMEM((CHUNKS, NX, NX, part, GROUP * HEAD_DIM), bf16),
            pltpu.VMEM((NX * part, out_cols), f32),
            pltpu.VMEM((CHUNKS, 4, part, out_cols), bf16),
            pltpu.SemaphoreType.DMA((5,)),
            pltpu.SemaphoreType.DMA((copies,)),
            pltpu.SemaphoreType.DMA((copies,)),
        ],
        compiler_params=pltpu.CompilerParams(
            collective_id=0, has_side_effects=True, vmem_limit_bytes=60 * 1024 * 1024
        ),
        name="tick",
    )(lengths.T, norm_gain, states[0], w_in[0], w_out[0])
    return moved[None]


def solution(mesh):
    n_pipe = mesh.shape["pipe"]
    n_y = mesh.shape["ctx"] // NX
    finer = Mesh(mesh.devices.reshape(n_pipe, n_y, NX), ("pipe", "ctx_y", "ctx_x"))
    ctx = ("ctx_y", "ctx_x")
    placed = (
        P("pipe", ctx, None),
        P("pipe", None),
        P("pipe", ctx, None),
        P("pipe", ctx, None),
        P(),
    )
    return jax.shard_map(
        body, mesh=finer, in_specs=placed, out_specs=P("pipe", ctx, None), check_vma=False
    )
```

```python
import functools
import math

import jax
import jax.numpy as jnp
from jax import lax
from jax.experimental import pallas as pl
from jax.experimental.pallas import tpu as pltpu
from jax.sharding import Mesh
from jax.sharding import PartitionSpec as P

HEAD_DIM = 64
HEADS = 16
KV_HEADS = 4
GROUP = HEADS // KV_HEADS
NX = 4
CHUNKS = 2
WINDOW = 9

epsilon = 1e-05
rope_base = 500000.0
masked_score = -1e30
MESH = pl.DeviceIdType.MESH


def sine_cosine(angle):
    turns = jnp.floor(angle * (2.0 / math.pi) + 0.5)
    quarter = turns.astype(jnp.int32)
    rest = angle - turns * 1.5703125
    rest = rest - turns * 4.837512969970703125e-4
    rest = rest - turns * 7.54978995489188216e-8
    z = rest * rest
    sine = ((-1.9515295891e-4 * z + 8.3321608736e-3) * z - 1.6666654611e-1) * z * rest + rest
    cosine = (
        (2.443315711809948e-5 * z - 1.388731625493765e-3) * z + 4.166664568298827e-2
    ) * z * z - 0.5 * z + 1.0
    odd = (quarter & 1) == 1
    sine, cosine = jnp.where(odd, cosine, sine), jnp.where(odd, sine, cosine)
    sine = jnp.where((quarter & 2) == 2, -sine, sine)
    cosine = jnp.where(((quarter + 1) & 2) == 2, -cosine, cosine)
    return sine, cosine


def response_start(ends, spots):
    start = jnp.zeros_like(spots)
    for end in ends:
        start = jnp.maximum(start, jnp.where(spots >= end, end, 0))
    return start


def tick_kernel(
    n_pipe,
    n_y,
    lengths_hbm,
    gain_hbm,
    x_hbm,
    wi_hbm,
    wo_hbm,
    out,
    lengths,
    gain,
    xg,
    xn,
    wloc,
    wsp,
    wkv,
    wq,
    wo,
    trig,
    q_s,
    kv,
    v_one,
    att,
    acc,
    obuf,
    local_sem,
    send_sem,
    recv_sem,
):
    p = lax.axis_index("pipe")
    y = lax.axis_index("ctx_y")
    x = lax.axis_index("ctx_x")
    rows = xg.shape[1]
    half = rows // 2
    part = rows // CHUNKS
    depth = xg.shape[2]
    out_cols = acc.shape[1]
    span = NX * rows

    def xs(d):
        return lax.rem(x + (d + NX), NX)

    def ys(d):
        return lax.rem(y + (d + n_y), n_y)

    def ps(d):
        return lax.rem(p + (d + n_pipe), n_pipe)

    counter = [0]
    pending = []

    def send(src, dst, device, landing=None):
        k = counter[0]
        counter[0] += 1
        copy = pltpu.make_async_remote_copy(
            src_ref=src,
            dst_ref=dst,
            send_sem=send_sem.at[k],
            recv_sem=recv_sem.at[k],
            device_id=device,
            device_id_type=MESH,
        )
        copy.start()
        pending.append(copy)
        land = dst if landing is None else landing

        def arrive():
            pltpu.make_async_remote_copy(
                src_ref=land,
                dst_ref=land,
                send_sem=send_sem.at[k],
                recv_sem=recv_sem.at[k],
                device_id=device,
                device_id_type=MESH,
            ).wait_recv()

        return arrive

    load_w = pltpu.make_async_copy(wi_hbm, wloc, local_sem.at[0])
    load_x = pltpu.make_async_copy(x_hbm, xg.at[0], local_sem.at[1])
    own_cols = pl.ds(pl.multiple_of(x * out_cols, out_cols), out_cols)
    load_o = pltpu.make_async_copy(
        wo_hbm.at[:, own_cols], wo.at[y, x], local_sem.at[2]
    )
    load_g = pltpu.make_async_copy(gain_hbm, gain, local_sem.at[3])
    load_l = pltpu.make_async_copy(lengths_hbm, lengths, local_sem.at[4])
    load_w.start()
    load_x.start()

    barrier = pltpu.get_barrier_semaphore()
    peers = [(p, y, xs(d)) for d in (1, 2, 3)]
    peers += [(p, ys(d), x) for d in (1, -1, -2)]
    for peer in peers + [(ps(-1), y, xs(d)) for d in range(NX)]:
        pl.semaphore_signal(barrier, inc=1, device_id=peer, device_id_type=MESH)
    load_l.start()
    load_g.start()
    load_o.start()

    load_w.wait()
    w_rows = wloc.shape[0]
    lane_w = lax.broadcasted_iota(jnp.int32, (w_rows, 128), 1)
    q_width = HEADS * HEAD_DIM
    g_width = GROUP * HEAD_DIM
    for t in range(NX):
        k_tile = wloc[:, q_width + 128 * (t // 2) : q_width + 128 * (t // 2) + 128]
        v_at = q_width + KV_HEADS * HEAD_DIM + 128 * (t // 2)
        v_tile = wloc[:, v_at : v_at + 128]
        k_tile = k_tile.astype(jnp.float32)
        v_tile = v_tile.astype(jnp.float32)
        if t % 2 == 0:
            v_tile = pltpu.roll(v_tile, 64, 1)
        else:
            k_tile = pltpu.roll(k_tile, 64, 1)
        wsp[t] = jnp.where(lane_w < 64, k_tile, v_tile).astype(jnp.bfloat16)

    def q_cols(d):
        return pl.ds(pl.multiple_of(xs(d) * g_width, g_width), g_width)

    wkv[y, x] = wsp[x]
    wq[y, x] = wloc[:, q_cols(0)]
    load_x.wait()
    with jax.named_scope("barrier"):
        pl.semaphore_wait(barrier, len(peers) + NX)

    north, south = (p, ys(1), x), (p, ys(-1), x)
    toward = {1: north, -1: south}
    reach = n_y // 2
    order = ((0, 1), (0, -1), (-1, 1), (-1, -1), (1, 1), (1, -1), (2, 1), (2, -1))
    only_south = ((0, -1), (-1, -1), (1, -1), (2, -1))
    shared = ((0, 1), (1, -1), (-1, 1), (2, -1))

    def ring_send(buf, d, way, step):
        source = buf.at[ys(-way * step), xs(d)]
        return send(source, source, toward[way], buf.at[ys(-way * (step + 1)), xs(d)])

    def ring_step(buf, final, step, arrivals):
        result = {}
        for key in order:
            if key not in arrivals:
                continue
            arrivals[key]()
            if step + 1 < reach - 1 or (step + 1 == reach - 1 and key in final):
                result[key] = ring_send(buf, *key, step + 1)
        return result

    def ring_own(buf):
        return {(0, way): ring_send(buf, 0, way, 0) for way in (1, -1)}

    def exchange(buf, source):
        return {
            -d % NX: send(source(d), buf.at[y, x], (p, y, xs(d)), buf.at[y, xs(-d)])
            for d in (1, -1, 2)
        }

    def ring_join(buf, landed, ring):
        for d in (-1, 1, 2):
            landed[d % NX]()
            for way in (1, -1):
                ring[d, way] = ring_send(buf, d, way, 0)

    kv_ring = ring_own(wkv)
    kv_in = exchange(wkv, lambda d: wsp.at[xs(d)])
    wq_ring = ring_own(wq)
    wq_in = exchange(wq, lambda d: wloc.at[:, q_cols(d)])
    first, second = pl.ds(0, half), pl.ds(half, half)
    up, down = (p, y, xs(1)), (p, y, xs(-1))
    x_up_a = send(xg.at[0, first], xg.at[1, first], up)
    x_down_b = send(xg.at[0, second], xg.at[2, second], down)
    x_up_b = send(xg.at[0, second], xg.at[1, second], up)
    x_down_a = send(xg.at[0, first], xg.at[2, first], down)

    load_l.wait()
    load_g.wait()
    ends = []
    total = 0
    for i in range(lengths.shape[0]):
        total = total + lengths[i, p]
        ends.append(total)
    deltas = (0, -1, 1, 2)
    lane = lax.broadcasted_iota(jnp.int32, (rows, 128), 1)
    row = lax.broadcasted_iota(jnp.int32, (rows, 128), 0)
    half_dim = HEAD_DIM // 2
    turn = lax.broadcasted_iota(jnp.int32, (8, 128), 1) & (half_dim - 1)
    inverse = jnp.zeros((8, 128), jnp.float32)
    for i in range(half_dim):
        inverse = jnp.where(turn == i, rope_base ** (-2.0 * i / HEAD_DIM), inverse)

    def make_trig(slot):
        spots = y * span + xs(deltas[slot]) * rows + row
        place_in = (spots - response_start(ends, spots)).astype(jnp.float32)
        sine, cosine = sine_cosine(place_in * inverse[:1])
        trig[slot, 0] = cosine
        trig[slot, 1] = jnp.where((lane & 63) < 32, -sine, sine)

    norm_rows = 32

    def normalize(slot):
        def step(i, carry):
            at = pl.ds(pl.multiple_of(i * norm_rows, norm_rows), norm_rows)
            wide = xg[slot, at, :].astype(jnp.float32)
            scale = lax.rsqrt(jnp.mean(wide * wide, -1, keepdims=True) + epsilon)
            to = pl.ds(pl.multiple_of(slot * rows + i * norm_rows, norm_rows), norm_rows)
            xn[to, :] = (wide * scale * gain[...]).astype(jnp.bfloat16)
            return carry

        lax.fori_loop(0, rows // norm_rows, step, 0, unroll=2)

    with jax.named_scope("trig"):
        for slot in range(4):
            make_trig(slot)
    with jax.named_scope("norm0"):
        normalize(0)
    def rotated(tile, slot):
        partner = jnp.where((lane & 63) < 32, pltpu.roll(tile, 96, 1), pltpu.roll(tile, 32, 1))
        return tile * trig[slot, 0] + partner * trig[slot, 1]

    def project(slot, count, buf):
        return jnp.dot(
            xn[slot * rows : (slot + count) * rows, :],
            buf[...].reshape(depth, buf.shape[3]),
            preferred_element_type=jnp.float32,
        )

    def project_kv(slot, count):
        proj = project(slot, count, wkv)
        arrivals = []
        for i in range(count):
            own = proj[i * rows : (i + 1) * rows]
            block = xs(deltas[slot + i])
            own = jnp.where(lane < 64, rotated(own, slot + i), own)
            kv[2 * NX + block] = own.astype(jnp.bfloat16)
            arrivals.append(send(kv.at[2 * NX + block], kv.at[NX + block], north))
        return arrivals

    def project_q(slot, count):
        proj = project(slot, count, wq)
        for i in range(count):
            own = proj[i * rows : (i + 1) * rows]
            block = xs(deltas[slot + i])
            for t in range(GROUP // 2):
                tile = rotated(own[:, 128 * t : 128 * (t + 1)], slot + i) * HEAD_DIM**-0.5
                q_s[block, 2 * t] = jnp.where(lane < 64, tile, 0.0).astype(jnp.bfloat16)
                q_s[block, 2 * t + 1] = jnp.where(
                    lane < 64, pltpu.roll(tile, 64, 1), 0.0
                ).astype(jnp.bfloat16)

    with jax.named_scope("kv_join"):
        ring_join(wkv, kv_in, kv_ring)
    with jax.named_scope("wq_join"):
        ring_join(wq, wq_in, wq_ring)
    with jax.named_scope("kv_ring0"):
        kv_ring = ring_step(wkv, only_south, 0, kv_ring)
    with jax.named_scope("wq_ring0"):
        wq_ring = ring_step(wq, only_south, 0, wq_ring)
    middle = range(1, reach - 1)
    for step in middle[:1]:
        with jax.named_scope("kv_ring1"):
            kv_ring = ring_step(wkv, only_south, step, kv_ring)
    with jax.named_scope("x_first"):
        x_up_a()
        x_far_a = send(xg.at[1, first], xg.at[3, first], up)
        x_down_b()
        x_far_b = send(xg.at[2, second], xg.at[3, second], down)

    def o_cols(d):
        return pl.ds(pl.multiple_of(xs(d) * out_cols, out_cols), out_cols)

    wo_in = exchange(wo, lambda d: wo_hbm.at[:, o_cols(d)])
    for step in middle[1:]:
        with jax.named_scope("kv_ring2"):
            kv_ring = ring_step(wkv, only_south, step, kv_ring)
    for step in middle[:1]:
        with jax.named_scope("wq_ring1"):
            wq_ring = ring_step(wq, only_south, step, wq_ring)
    with jax.named_scope("kv_ring3"):
        ring_step(wkv, only_south, reach - 1, kv_ring)
    with jax.named_scope("x_second"):
        x_up_b()
        x_down_a()
    with jax.named_scope("norm12"):
        normalize(1)
        normalize(2)
    with jax.named_scope("kv012"):
        near = project_kv(0, 3)
    for step in middle[1:]:
        with jax.named_scope("wq_ring2"):
            wq_ring = ring_step(wq, only_south, step, wq_ring)
    load_o.wait()
    wo_ring = ring_own(wo)
    far = []
    with jax.named_scope("kv_near"):
        for slot in range(3):
            near[slot]()
            block = xs(deltas[slot])
            far.append(send(kv.at[NX + block], kv.at[block], north))
    with jax.named_scope("x_far"):
        x_far_a()
        x_far_b()
    with jax.named_scope("norm3"):
        normalize(3)
    with jax.named_scope("kv3"):
        near += project_kv(3, 1)
    block = xs(deltas[3])
    far.append(send(kv.at[2 * NX + block], kv.at[block], (p, ys(2), x)))
    with jax.named_scope("wq_ring3"):
        ring_step(wq, only_south, reach - 1, wq_ring)
    with jax.named_scope("q012"):
        project_q(0, 3)
    with jax.named_scope("wo_join"):
        ring_join(wo, wo_in, wo_ring)
    with jax.named_scope("q3"):
        project_q(3, 1)
    with jax.named_scope("kv_far"):
        near[3]()
        for arrive in far:
            arrive()
    with jax.named_scope("v_one"):
        for b in range(3 * NX):
            v_one[b] = jnp.where(lane < 64, 1.0, kv[b].astype(jnp.float32)).astype(jnp.bfloat16)

    lane_p = lax.broadcasted_iota(jnp.int32, (part, 128), 1)
    row_p = lax.broadcasted_iota(jnp.int32, (part, 128), 0)

    def attend(i, j):
        queries = q_s[j, :, i * part : (i + 1) * part, :].reshape(GROUP * part, 128)
        window = kv[j : j + WINDOW].reshape(WINDOW * rows, 128)
        values = v_one[j : j + WINDOW].reshape(WINDOW * rows, 128)
        scores = lax.dot_general(
            queries, window, (((1,), (1,)), ((), ())), preferred_element_type=jnp.float32
        )
        spots = y * span + j * rows + i * part + row_p
        start = response_start(ends, spots)
        allowed = []
        for c in range(WINDOW):
            keys = y * span + (j + c - 2 * NX) * rows + lane_p
            inside = keys >= start
            if c == WINDOW - 1:
                inside = inside & (keys <= spots)
            allowed.append(inside)
        allowed = jnp.concatenate(allowed, 1)
        scores = jnp.where(
            allowed[None], scores.reshape(GROUP, part, WINDOW * rows), masked_score
        )
        probs = jnp.exp(scores - jnp.max(scores, -1, keepdims=True))
        mixed = jnp.dot(
            probs.astype(jnp.bfloat16).reshape(GROUP * part, WINDOW * rows),
            values,
            preferred_element_type=jnp.float32,
        )
        turned = pltpu.roll(mixed, 64, 1)
        tiles = []
        for t in range(GROUP // 2):
            even = slice(2 * t * part, (2 * t + 1) * part)
            odd = slice((2 * t + 1) * part, (2 * t + 2) * part)
            tiles.append(
                jnp.where(lane_p < 64, turned[even] / mixed[even], mixed[odd] / turned[odd])
            )
        att[i, x, j] = jnp.concatenate(tiles, 1).astype(jnp.bfloat16)

    low, high = pl.ds(0, NX // 2), pl.ds(NX // 2, NX // 2)

    def att_start(i):
        return (
            send(att.at[i, x, low], att.at[i, x, low], up, att.at[i, xs(-1), low]),
            send(att.at[i, x, high], att.at[i, x, high], down, att.at[i, xs(1), high]),
            send(att.at[i, x, high], att.at[i, x, high], up, att.at[i, xs(-1), high]),
            send(att.at[i, x, low], att.at[i, x, low], down, att.at[i, xs(1), low]),
        )

    def att_pass(i, arrivals):
        arrivals[0]()
        piece = att.at[i, xs(-1), low]
        far_low = send(piece, piece, up, att.at[i, xs(2), low])
        arrivals[1]()
        piece = att.at[i, xs(1), high]
        far_high = send(piece, piece, down, att.at[i, xs(2), high])
        return (arrivals[2], arrivals[3], far_low, far_high)

    def finish(i):
        weight = wo[...].reshape(q_width, out_cols)
        result = None
        for h in range(NX):
            term = jnp.dot(
                att[i, h].reshape(NX * part, g_width),
                weight[h * g_width : (h + 1) * g_width],
                preferred_element_type=jnp.float32,
            )
            result = term if result is None else result + term
        acc[...] = result
        arrivals = []
        for slot in (3, 2, 1, 0):
            d = deltas[slot]
            j = xs(d)
            kept = xg[slot, i * part : (i + 1) * part, own_cols].astype(jnp.float32)
            at = pl.ds(pl.multiple_of(j * part, part), part)
            obuf[i, slot] = (acc[at, :] + kept).astype(jnp.bfloat16)
            from_cols = pl.ds(pl.multiple_of(xs(-d) * out_cols, out_cols), out_cols)
            there = pl.ds(i * part, part)
            arrivals.append(
                send(
                    obuf.at[i, slot],
                    out.at[there, own_cols],
                    (ps(1), y, j),
                    out.at[there, from_cols],
                )
            )
        return arrivals

    with jax.named_scope("attend0a"):
        attend(0, 0)
        attend(0, 1)
    with jax.named_scope("wo0"):
        wo_ring = ring_step(wo, shared, 0, wo_ring)
    with jax.named_scope("attend0b"):
        attend(0, 2)
        attend(0, 3)
    arrivals_0 = att_start(0)
    with jax.named_scope("attend1a"):
        attend(1, 0)
        attend(1, 1)
    for step in range(1, reach - 2):
        with jax.named_scope("wo1"):
            wo_ring = ring_step(wo, shared, step, wo_ring)
    with jax.named_scope("attend1b"):
        attend(1, 2)
        attend(1, 3)
    with jax.named_scope("pass0"):
        arrivals_0 = att_pass(0, arrivals_0)
    arrivals_1 = att_start(1)
    with jax.named_scope("wo2"):
        if reach > 2:
            wo_ring = ring_step(wo, shared, reach - 2, wo_ring)
    with jax.named_scope("att0_in"):
        for arrive in arrivals_0:
            arrive()
    with jax.named_scope("pass1"):
        arrivals_1 = att_pass(1, arrivals_1)
    with jax.named_scope("wo3"):
        wo_ring = ring_step(wo, shared, reach - 1, wo_ring)
    with jax.named_scope("finish0"):
        last = finish(0)
    with jax.named_scope("att1_in"):
        for arrive in arrivals_1:
            arrive()
    with jax.named_scope("finish1"):
        last += finish(1)
    with jax.named_scope("out_in"):
        for arrive in last:
            arrive()
    with jax.named_scope("wait_send"):
        for copy in pending:
            copy.wait_send()


def body(states, norm_gain, w_in, w_out, lengths):
    rows, depth = states.shape[1:]
    w_rows = w_in.shape[1]
    o_rows = w_out.shape[1]
    out_cols = depth // NX
    n_pipe = lax.axis_size("pipe")
    n_y = lax.axis_size("ctx_y")
    part = rows // CHUNKS
    copies = 160
    bf16, f32 = jnp.bfloat16, jnp.float32
    moved = pl.pallas_call(
        functools.partial(tick_kernel, n_pipe, n_y),
        out_shape=pltpu.VMEM((rows, depth), bf16),
        in_specs=[
            pl.BlockSpec(memory_space=pl.ANY),
            pl.BlockSpec(memory_space=pl.ANY),
            pl.BlockSpec(memory_space=pl.ANY),
            pl.BlockSpec(memory_space=pl.ANY),
            pl.BlockSpec(memory_space=pl.ANY),
        ],
        out_specs=pl.BlockSpec(memory_space=pltpu.VMEM),
        scratch_shapes=[
            pltpu.SMEM(lengths.shape[::-1], jnp.int32),
            pltpu.VMEM((1, depth), f32),
            pltpu.VMEM((4, rows, depth), bf16),
            pltpu.VMEM((4 * rows, depth), bf16),
            pltpu.VMEM((w_rows, w_in.shape[2]), bf16),
            pltpu.VMEM((NX, w_rows, 128), bf16),
            pltpu.VMEM((n_y, NX, w_rows, 128), bf16),
            pltpu.VMEM((n_y, NX, w_rows, GROUP * HEAD_DIM), bf16),
            pltpu.VMEM((n_y, NX, o_rows, out_cols), bf16),
            pltpu.VMEM((4, 2, rows, 128), f32),
            pltpu.VMEM((NX, GROUP, rows, 128), bf16),
            pltpu.VMEM((3 * NX, rows, 128), bf16),
            pltpu.VMEM((3 * NX, rows, 128), bf16),
            pltpu.VMEM((CHUNKS, NX, NX, part, GROUP * HEAD_DIM), bf16),
            pltpu.VMEM((NX * part, out_cols), f32),
            pltpu.VMEM((CHUNKS, 4, part, out_cols), bf16),
            pltpu.SemaphoreType.DMA((5,)),
            pltpu.SemaphoreType.DMA((copies,)),
            pltpu.SemaphoreType.DMA((copies,)),
        ],
        compiler_params=pltpu.CompilerParams(
            collective_id=0, has_side_effects=True, vmem_limit_bytes=60 * 1024 * 1024
        ),
        name="tick",
    )(lengths.T, norm_gain, states[0], w_in[0], w_out[0])
    return moved[None]


def solution(mesh):
    n_pipe = mesh.shape["pipe"]
    n_y = mesh.shape["ctx"] // NX
    finer = Mesh(mesh.devices.reshape(n_pipe, n_y, NX), ("pipe", "ctx_y", "ctx_x"))
    ctx = ("ctx_y", "ctx_x")
    placed = (
        P("pipe", ctx, None),
        P("pipe", None),
        P("pipe", ctx, None),
        P("pipe", ctx, None),
        P(),
    )
    return jax.shard_map(
        body, mesh=finer, in_specs=placed, out_specs=P("pipe", ctx, None), check_vma=False
    )
```

```python
import functools
import math

import jax
import jax.numpy as jnp
from jax import lax
from jax.experimental import pallas as pl
from jax.experimental.pallas import tpu as pltpu
from jax.sharding import Mesh
from jax.sharding import PartitionSpec as P

HEAD_DIM = 64
HEADS = 16
KV_HEADS = 4
GROUP = HEADS // KV_HEADS
NX = 4
CHUNKS = 2
WINDOW = 9

epsilon = 1e-05
rope_base = 500000.0
masked_score = -1e30
MESH = pl.DeviceIdType.MESH


def sine_cosine(angle):
    turns = jnp.floor(angle * (2.0 / math.pi) + 0.5)
    quarter = turns.astype(jnp.int32)
    rest = angle - turns * 1.5703125
    rest = rest - turns * 4.837512969970703125e-4
    rest = rest - turns * 7.54978995489188216e-8
    z = rest * rest
    sine = ((-1.9515295891e-4 * z + 8.3321608736e-3) * z - 1.6666654611e-1) * z * rest + rest
    cosine = (
        (2.443315711809948e-5 * z - 1.388731625493765e-3) * z + 4.166664568298827e-2
    ) * z * z - 0.5 * z + 1.0
    odd = (quarter & 1) == 1
    sine, cosine = jnp.where(odd, cosine, sine), jnp.where(odd, sine, cosine)
    sine = jnp.where((quarter & 2) == 2, -sine, sine)
    cosine = jnp.where(((quarter + 1) & 2) == 2, -cosine, cosine)
    return sine, cosine


def response_start(ends, spots):
    start = jnp.zeros_like(spots)
    for end in ends:
        start = jnp.maximum(start, jnp.where(spots >= end, end, 0))
    return start


def tick_kernel(
    n_pipe,
    n_y,
    lengths_hbm,
    gain_hbm,
    x_hbm,
    wi_hbm,
    wo_hbm,
    out,
    lengths,
    gain,
    xg,
    xn,
    wloc,
    wsp,
    wkv,
    wq,
    wo,
    trig,
    masks,
    q_s,
    kv,
    v_one,
    att,
    acc,
    obuf,
    local_sem,
    send_sem,
    recv_sem,
):
    p = lax.axis_index("pipe")
    y = lax.axis_index("ctx_y")
    x = lax.axis_index("ctx_x")
    rows = xg.shape[1]
    half = rows // 2
    part = rows // CHUNKS
    depth = xg.shape[2]
    out_cols = acc.shape[1]
    span = NX * rows

    def xs(d):
        return lax.rem(x + (d + NX), NX)

    def ys(d):
        return lax.rem(y + (d + n_y), n_y)

    def ps(d):
        return lax.rem(p + (d + n_pipe), n_pipe)

    slots = {}
    sources = {}

    def copy_of(name, src, dst, device):
        k = slots.setdefault(name, len(slots))
        return pltpu.make_async_remote_copy(
            src_ref=src,
            dst_ref=dst,
            send_sem=send_sem.at[k],
            recv_sem=recv_sem.at[k],
            device_id=device,
            device_id_type=MESH,
        )

    def send(name, src, device, dst=None):
        sources[name] = src
        copy_of(name, src(), src() if dst is None else dst(), device).start()

    def land(name, dst):
        copy_of(name, dst, dst, (p, y, x)).wait_recv()

    load_w = pltpu.make_async_copy(wi_hbm, wloc, local_sem.at[0])
    load_x = pltpu.make_async_copy(x_hbm, xg.at[0], local_sem.at[1])
    own_cols = pl.ds(pl.multiple_of(x * out_cols, out_cols), out_cols)
    load_o = pltpu.make_async_copy(
        wo_hbm.at[:, own_cols], wo.at[y, x], local_sem.at[2]
    )
    load_g = pltpu.make_async_copy(gain_hbm, gain, local_sem.at[3])
    load_l = pltpu.make_async_copy(lengths_hbm, lengths, local_sem.at[4])
    load_w.start()
    load_x.start()

    barrier = pltpu.get_barrier_semaphore()
    peers = [(p, y, xs(d)) for d in (1, 2, 3)]
    peers += [(p, ys(d), x) for d in (1, -1)]
    peers += [(p, ys(-2), x)]
    for peer in peers + [(ps(-1), y, xs(d)) for d in range(NX)]:
        pl.semaphore_signal(barrier, inc=1, device_id=peer, device_id_type=MESH)
    load_l.start()
    load_g.start()
    load_o.start()

    load_w.wait()
    w_rows = wloc.shape[0]
    lane_w = lax.broadcasted_iota(jnp.int32, (w_rows, 128), 1)
    q_width = HEADS * HEAD_DIM
    g_width = GROUP * HEAD_DIM
    for t in range(NX):
        k_tile = wloc[:, q_width + 128 * (t // 2) : q_width + 128 * (t // 2) + 128]
        v_at = q_width + KV_HEADS * HEAD_DIM + 128 * (t // 2)
        v_tile = wloc[:, v_at : v_at + 128]
        k_tile = k_tile.astype(jnp.float32)
        v_tile = v_tile.astype(jnp.float32)
        if t % 2 == 0:
            v_tile = pltpu.roll(v_tile, 64, 1)
        else:
            k_tile = pltpu.roll(k_tile, 64, 1)
        wsp[t] = jnp.where(lane_w < 64, k_tile, v_tile).astype(jnp.bfloat16)

    def q_cols(d):
        return pl.ds(pl.multiple_of(xs(d) * g_width, g_width), g_width)

    wkv[y, x] = wsp[x]
    wq[y, x] = wloc[:, q_cols(0)]
    load_x.wait()
    with jax.named_scope("barrier"):
        pl.semaphore_wait(barrier, len(peers) + NX)

    north, south = (p, ys(1), x), (p, ys(-1), x)
    up, down = (p, y, xs(1)), (p, y, xs(-1))
    toward = {1: north, -1: south}
    reach = n_y // 2
    order = ((0, 1), (0, -1), (-1, 1), (-1, -1), (1, 1), (1, -1), (2, 1), (2, -1))
    only_south = ((0, -1), (-1, -1), (1, -1), (2, -1))
    rings = {"kv": (wkv, only_south), "q": (wq, only_south), "o": (wo, only_south)}

    def ring_send(ring, d, way, step):
        buf = rings[ring][0]
        send(
            (ring, d, way, step),
            lambda: buf.at[ys(-way * step), xs(d)],
            toward[way],
        )

    def ring_step(ring, step, pieces=order):
        buf, final = rings[ring]
        if not 0 <= step < reach:
            return
        with jax.named_scope(f"{ring}_ring{step}"):
            for d, way in pieces:
                if step == reach - 1 and (d, way) not in final:
                    continue
                land((ring, d, way, step), buf.at[ys(-way * (step + 1)), xs(d)])
                if step + 1 < reach - 1 or (step + 1 == reach - 1 and (d, way) in final):
                    ring_send(ring, d, way, step + 1)

    def ring_steps(ring, *steps):
        for step in steps:
            if 0 <= step < reach - 1:
                ring_step(ring, step)

    def ring_own(ring):
        for way in (1, -1):
            ring_send(ring, 0, way, 0)

    def exchange(ring, source):
        buf = rings[ring][0]
        for d in (1, -1, 2):
            send((ring, d), lambda d=d: source(d), (p, y, xs(d)), lambda: buf.at[y, x])

    def ring_join(ring, *ways):
        with jax.named_scope(f"{ring}_join"):
            for d in (1, -1, 2):
                land((ring, d), rings[ring][0].at[y, xs(-d)])
                e = d if d == 2 else -d
                for way in ways:
                    ring_send(ring, e, way, 0)

    first, second = pl.ds(0, half), pl.ds(half, half)

    def x_start():
        send("x_up_a", lambda: xg.at[0, first], up, lambda: xg.at[1, first])
        send("x_down_b", lambda: xg.at[0, second], down, lambda: xg.at[2, second])
        send("x_up_b", lambda: xg.at[0, second], up, lambda: xg.at[1, second])
        send("x_down_a", lambda: xg.at[0, first], down, lambda: xg.at[2, first])

    def x_pass():
        with jax.named_scope("x_first"):
            land("x_up_a", xg.at[1, first])
            send("x_far_a", lambda: xg.at[1, first], up, lambda: xg.at[3, first])
            land("x_down_b", xg.at[2, second])
            send("x_far_b", lambda: xg.at[2, second], down, lambda: xg.at[3, second])

    def x_second():
        with jax.named_scope("x_second"):
            land("x_up_b", xg.at[1, second])
            land("x_down_a", xg.at[2, first])

    def x_far():
        with jax.named_scope("x_far"):
            land("x_far_a", xg.at[3, first])
            land("x_far_b", xg.at[3, second])

    def kv_exchange():
        exchange("kv", lambda d: wsp.at[xs(d)])

    def q_exchange():
        exchange("q", lambda d: wloc.at[:, q_cols(d)])

    def o_exchange():
        exchange("o", lambda d: wo_hbm.at[:, o_cols(d)])

    def o_cols(d):
        return pl.ds(pl.multiple_of(xs(d) * out_cols, out_cols), out_cols)

    load_l.wait()
    load_g.wait()
    ends = []
    total = 0
    for i in range(lengths.shape[0]):
        total = total + lengths[i, p]
        ends.append(total)
    deltas = (0, -1, 1, 2)
    lane = lax.broadcasted_iota(jnp.int32, (rows, 128), 1)
    row = lax.broadcasted_iota(jnp.int32, (rows, 128), 0)
    half_dim = HEAD_DIM // 2
    turn = lax.broadcasted_iota(jnp.int32, (8, 128), 1) & (half_dim - 1)
    inverse = jnp.zeros((8, 128), jnp.float32)
    for i in range(half_dim):
        inverse = jnp.where(turn == i, rope_base ** (-2.0 * i / HEAD_DIM), inverse)

    def make_trig(slot):
        spots = y * span + xs(deltas[slot]) * rows + row
        place_in = (spots - response_start(ends, spots)).astype(jnp.float32)
        sine, cosine = sine_cosine(place_in * inverse[:1])
        trig[slot, 0] = cosine
        trig[slot, 1] = jnp.where((lane & 63) < 32, -sine, sine)

    norm_rows = 32

    def normalize(slot):
        def step(i, carry):
            at = pl.ds(pl.multiple_of(i * norm_rows, norm_rows), norm_rows)
            wide = xg[slot, at, :].astype(jnp.float32)
            scale = lax.rsqrt(jnp.mean(wide * wide, -1, keepdims=True) + epsilon)
            to = pl.ds(pl.multiple_of(slot * rows + i * norm_rows, norm_rows), norm_rows)
            xn[to, :] = (wide * scale * gain[...]).astype(jnp.bfloat16)
            return carry

        lax.fori_loop(0, rows // norm_rows, step, 0, unroll=2)

    def rotated(tile, slot):
        partner = jnp.where((lane & 63) < 32, pltpu.roll(tile, 96, 1), pltpu.roll(tile, 32, 1))
        return tile * trig[slot, 0] + partner * trig[slot, 1]

    def project(slot, count, buf):
        return jnp.dot(
            xn[slot * rows : (slot + count) * rows, :],
            buf[...].reshape(depth, buf.shape[3]),
            preferred_element_type=jnp.float32,
        )

    def own_kv(slot):
        return kv.at[2 * NX + xs(deltas[slot])]

    def near_kv(slot):
        return kv.at[NX + xs(deltas[slot])]

    def far_kv(slot):
        return kv.at[xs(deltas[slot])]

    def project_kv(slot, count):
        with jax.named_scope(f"kv{slot}"):
            proj = project(slot, count, wkv)
            for i in range(count):
                own = proj[i * rows : (i + 1) * rows]
                own = jnp.where(lane < 64, rotated(own, slot + i), own)
                kv[2 * NX + xs(deltas[slot + i])] = own.astype(jnp.bfloat16)
                send(
                    ("far", slot + i),
                    lambda i=i: own_kv(slot + i),
                    (p, ys(2), x),
                    lambda i=i: far_kv(slot + i),
                )
                send(
                    ("near", slot + i),
                    lambda i=i: own_kv(slot + i),
                    north,
                    lambda i=i: near_kv(slot + i),
                )

    def project_q(slot, count):
        proj = project(slot, count, wq)
        for i in range(count):
            own = proj[i * rows : (i + 1) * rows]
            block = xs(deltas[slot + i])
            for t in range(GROUP // 2):
                tile = rotated(own[:, 128 * t : 128 * (t + 1)], slot + i) * HEAD_DIM**-0.5
                q_s[block, 2 * t] = jnp.where(lane < 64, tile, 0.0).astype(jnp.bfloat16)
                q_s[block, 2 * t + 1] = jnp.where(
                    lane < 64, pltpu.roll(tile, 64, 1), 0.0
                ).astype(jnp.bfloat16)

    lane_p = lax.broadcasted_iota(jnp.int32, (part, 128), 1)
    row_p = lax.broadcasted_iota(jnp.int32, (part, 128), 0)

    def make_masks(i):
        def one(j, carry):
            spots = y * span + j * rows + i * part + row_p
            start = response_start(ends, spots)
            for c in range(WINDOW):
                keys = y * span + (j + c - 2 * NX) * rows + lane_p
                inside = keys >= start
                if c == WINDOW - 1:
                    inside = inside & (keys <= spots)
                masks[i, j, :, c * rows : (c + 1) * rows] = jnp.where(inside, 0.0, masked_score)
            return carry

        lax.fori_loop(0, NX, one, 0)

    def prepare():
        with jax.named_scope("trig"):
            for slot in range(4):
                make_trig(slot)
        with jax.named_scope("norm0"):
            normalize(0)
        with jax.named_scope("masks"):
            for i in range(CHUNKS):
                make_masks(i)

    def norms(*which):
        with jax.named_scope("norms"):
            for slot in which:
                normalize(slot)

    def last_block():
        x_far()
        norms(3)
        project_kv(3, 1)

    def queries_of(slot, count):
        with jax.named_scope(f"q{slot}"):
            project_q(slot, count)

    late = lax.rem(p + p // (n_pipe - 2), 2) == 1
    ring_own("kv")
    kv_exchange()
    ring_own("q")
    q_exchange()

    @pl.when(jnp.logical_not(late))
    def _():
        x_start()

    prepare()
    ring_join("kv", 1, -1)

    @pl.when(late)
    def _():
        x_start()

    ring_join("q", 1, -1)
    ring_steps("kv", 0)
    ring_steps("q", 0)
    ring_steps("kv", 1)
    x_pass()
    o_exchange()
    ring_steps("kv", *range(2, reach))
    ring_steps("q", 1)
    ring_step("kv", reach - 1)
    x_second()
    norms(1, 2)
    project_kv(0, 3)
    ring_steps("q", *range(2, reach))
    last_block()
    going_north = ((-1, 1), (1, 1), (2, 1))
    going_south = ((-1, -1), (1, -1), (2, -1))
    load_o.wait()
    ring_send("o", 0, -1, 0)
    ring_join("o", -1)
    ring_step("q", reach - 1)
    queries_of(0, 3)
    queries_of(3, 1)
    with jax.named_scope("kv_near"):
        for slot in range(4):
            land(("near", slot), near_kv(slot))
    for d in (0, -1, 1, 2):
        ring_send("o", d, 1, 0)
    ring_step("o", 0, ((0, -1),) + going_south)
    with jax.named_scope("kv_far"):
        for slot in range(4):
            land(("far", slot), far_kv(slot))
    with jax.named_scope("v_one"):
        for b in range(3 * NX):
            v_one[b] = jnp.where(lane < 64, 1.0, kv[b].astype(jnp.float32)).astype(jnp.bfloat16)

    def attend(i, j):
        queries = q_s[j, :, i * part : (i + 1) * part, :].reshape(GROUP * part, 128)
        window = kv[j : j + WINDOW].reshape(WINDOW * rows, 128)
        values = v_one[j : j + WINDOW].reshape(WINDOW * rows, 128)
        scores = lax.dot_general(
            queries, window, (((1,), (1,)), ((), ())), preferred_element_type=jnp.float32
        )
        scores = scores.reshape(GROUP, part, WINDOW * rows) + masks[i, j][None]
        probs = jnp.exp(scores - jnp.max(scores, -1, keepdims=True))
        mixed = jnp.dot(
            probs.astype(jnp.bfloat16).reshape(GROUP * part, WINDOW * rows),
            values,
            preferred_element_type=jnp.float32,
        )
        turned = pltpu.roll(mixed, 64, 1)
        tiles = []
        for t in range(GROUP // 2):
            even = slice(2 * t * part, (2 * t + 1) * part)
            odd = slice((2 * t + 1) * part, (2 * t + 2) * part)
            tiles.append(
                jnp.where(lane_p < 64, turned[even] / mixed[even], mixed[odd] / turned[odd])
            )
        att[i, x, j] = jnp.concatenate(tiles, 1).astype(jnp.bfloat16)

    low, high = pl.ds(0, NX // 2), pl.ds(NX // 2, NX // 2)

    def piece(i, d, which):
        return att.at[i, xs(d), which]

    def att_start(i):
        send(("up_l", i), lambda: piece(i, 0, low), up)
        send(("down_h", i), lambda: piece(i, 0, high), down)
        send(("up_h", i), lambda: piece(i, 0, high), up)
        send(("down_l", i), lambda: piece(i, 0, low), down)

    def att_pass(i):
        with jax.named_scope(f"pass{i}"):
            land(("up_l", i), piece(i, -1, low))
            send(("far_l", i), lambda: piece(i, -1, low), up)
            land(("down_h", i), piece(i, 1, high))
            send(("far_h", i), lambda: piece(i, 1, high), down)

    def att_in(i):
        with jax.named_scope(f"att{i}_in"):
            land(("up_h", i), piece(i, -1, high))
            land(("down_l", i), piece(i, 1, low))
            land(("far_l", i), piece(i, 2, low))
            land(("far_h", i), piece(i, 2, high))

    def out_part(i, d):
        return out.at[pl.ds(i * part, part), o_cols(d)]

    def finish(i):
        weight = wo[...].reshape(q_width, out_cols)
        result = None
        for h in range(NX):
            term = jnp.dot(
                att[i, h].reshape(NX * part, g_width),
                weight[h * g_width : (h + 1) * g_width],
                preferred_element_type=jnp.float32,
            )
            result = term if result is None else result + term
        acc[...] = result
        for slot in (3, 2, 1, 0):
            j = xs(deltas[slot])
            kept = xg[slot, i * part : (i + 1) * part, own_cols].astype(jnp.float32)
            at = pl.ds(pl.multiple_of(j * part, part), part)
            obuf[i, slot] = (acc[at, :] + kept).astype(jnp.bfloat16)
            send(
                ("out", i, slot),
                lambda slot=slot: obuf.at[i, slot],
                (ps(1), y, j),
                lambda: out_part(i, 0),
            )

    def o_steps(step, pieces):
        if step < reach - 1:
            ring_step("o", step, pieces)

    with jax.named_scope("attend0a"):
        attend(0, 0)
        attend(0, 1)
    with jax.named_scope("attend0b"):
        attend(0, 2)
        attend(0, 3)
    att_start(0)
    with jax.named_scope("attend1a"):
        attend(1, 0)
        attend(1, 1)
    ring_step("o", 0, ((0, 1),) + going_north)
    o_steps(1, ((0, -1),) + going_south)
    with jax.named_scope("attend1b"):
        attend(1, 2)
        attend(1, 3)
    att_pass(0)
    att_start(1)
    o_steps(1, ((0, 1),) + going_north)
    for step in range(2, reach - 1):
        o_steps(step, ((0, -1),) + going_south)
    att_in(0)
    att_pass(1)
    for step in range(2, reach - 1):
        o_steps(step, ((0, 1),) + going_north)
    ring_step("o", reach - 1)
    with jax.named_scope("finish0"):
        finish(0)
    att_in(1)
    with jax.named_scope("finish1"):
        finish(1)
    with jax.named_scope("out_in"):
        for i in range(CHUNKS):
            for slot in (3, 2, 1, 0):
                land(("out", i, slot), out_part(i, -deltas[slot]))
    with jax.named_scope("wait_send"):
        for name, src in sources.items():
            copy_of(name, src(), src(), (p, y, x)).wait_send()


def body(states, norm_gain, w_in, w_out, lengths):
    rows, depth = states.shape[1:]
    w_rows = w_in.shape[1]
    o_rows = w_out.shape[1]
    out_cols = depth // NX
    n_pipe = lax.axis_size("pipe")
    n_y = lax.axis_size("ctx_y")
    part = rows // CHUNKS
    copies = 160
    bf16, f32 = jnp.bfloat16, jnp.float32
    moved = pl.pallas_call(
        functools.partial(tick_kernel, n_pipe, n_y),
        out_shape=pltpu.VMEM((rows, depth), bf16),
        in_specs=[
            pl.BlockSpec(memory_space=pl.ANY),
            pl.BlockSpec(memory_space=pl.ANY),
            pl.BlockSpec(memory_space=pl.ANY),
            pl.BlockSpec(memory_space=pl.ANY),
            pl.BlockSpec(memory_space=pl.ANY),
        ],
        out_specs=pl.BlockSpec(memory_space=pltpu.VMEM),
        scratch_shapes=[
            pltpu.SMEM(lengths.shape[::-1], jnp.int32),
            pltpu.VMEM((1, depth), f32),
            pltpu.VMEM((4, rows, depth), bf16),
            pltpu.VMEM((4 * rows, depth), bf16),
            pltpu.VMEM((w_rows, w_in.shape[2]), bf16),
            pltpu.VMEM((NX, w_rows, 128), bf16),
            pltpu.VMEM((n_y, NX, w_rows, 128), bf16),
            pltpu.VMEM((n_y, NX, w_rows, GROUP * HEAD_DIM), bf16),
            pltpu.VMEM((n_y, NX, o_rows, out_cols), bf16),
            pltpu.VMEM((4, 2, rows, 128), f32),
            pltpu.VMEM((CHUNKS, NX, part, WINDOW * rows), f32),
            pltpu.VMEM((NX, GROUP, rows, 128), bf16),
            pltpu.VMEM((3 * NX, rows, 128), bf16),
            pltpu.VMEM((3 * NX, rows, 128), bf16),
            pltpu.VMEM((CHUNKS, NX, NX, part, GROUP * HEAD_DIM), bf16),
            pltpu.VMEM((NX * part, out_cols), f32),
            pltpu.VMEM((CHUNKS, 4, part, out_cols), bf16),
            pltpu.SemaphoreType.DMA((5,)),
            pltpu.SemaphoreType.DMA((copies,)),
            pltpu.SemaphoreType.DMA((copies,)),
        ],
        compiler_params=pltpu.CompilerParams(
            collective_id=0, has_side_effects=True, vmem_limit_bytes=60 * 1024 * 1024
        ),
        name="tick",
    )(lengths.T, norm_gain, states[0], w_in[0], w_out[0])
    return moved[None]


def solution(mesh):
    n_pipe = mesh.shape["pipe"]
    n_y = mesh.shape["ctx"] // NX
    finer = Mesh(mesh.devices.reshape(n_pipe, n_y, NX), ("pipe", "ctx_y", "ctx_x"))
    ctx = ("ctx_y", "ctx_x")
    placed = (
        P("pipe", ctx, None),
        P("pipe", None),
        P("pipe", ctx, None),
        P("pipe", ctx, None),
        P(),
    )
    return jax.shard_map(
        body, mesh=finer, in_specs=placed, out_specs=P("pipe", ctx, None), check_vma=False
    )
```

```python
import functools
import math

import jax
import jax.numpy as jnp
from jax import lax
from jax.experimental import pallas as pl
from jax.experimental.pallas import tpu as pltpu
from jax.sharding import Mesh
from jax.sharding import PartitionSpec as P

HEAD_DIM = 64
HEADS = 16
KV_HEADS = 4
GROUP = HEADS // KV_HEADS
NX = 4
CHUNKS = 2
WINDOW = 9

epsilon = 1e-05
rope_base = 500000.0
masked_score = -1e30
MESH = pl.DeviceIdType.MESH


def sine_cosine(angle):
    turns = jnp.floor(angle * (2.0 / math.pi) + 0.5)
    quarter = turns.astype(jnp.int32)
    rest = angle - turns * 1.5703125
    rest = rest - turns * 4.837512969970703125e-4
    rest = rest - turns * 7.54978995489188216e-8
    z = rest * rest
    sine = ((-1.9515295891e-4 * z + 8.3321608736e-3) * z - 1.6666654611e-1) * z * rest + rest
    cosine = (
        (2.443315711809948e-5 * z - 1.388731625493765e-3) * z + 4.166664568298827e-2
    ) * z * z - 0.5 * z + 1.0
    odd = (quarter & 1) == 1
    sine, cosine = jnp.where(odd, cosine, sine), jnp.where(odd, sine, cosine)
    sine = jnp.where((quarter & 2) == 2, -sine, sine)
    cosine = jnp.where(((quarter + 1) & 2) == 2, -cosine, cosine)
    return sine, cosine


def response_start(ends, spots):
    start = jnp.zeros_like(spots)
    for end in ends:
        start = jnp.maximum(start, jnp.where(spots >= end, end, 0))
    return start


def tick_kernel(
    n_pipe,
    n_y,
    lengths_hbm,
    gain_hbm,
    x_hbm,
    wi_hbm,
    wo_hbm,
    out,
    lengths,
    gain,
    xg,
    xn,
    wloc,
    wsp,
    wkv,
    wq,
    wo,
    trig,
    masks,
    q_s,
    kv,
    v_one,
    att,
    acc,
    obuf,
    local_sem,
    send_sem,
    recv_sem,
):
    p = lax.axis_index("pipe")
    y = lax.axis_index("ctx_y")
    x = lax.axis_index("ctx_x")
    rows = xg.shape[1]
    half = rows // 2
    part = rows // CHUNKS
    depth = xg.shape[2]
    out_cols = acc.shape[1]
    span = NX * rows

    def xs(d):
        return lax.rem(x + (d + NX), NX)

    def ys(d):
        return lax.rem(y + (d + n_y), n_y)

    def ps(d):
        return lax.rem(p + (d + n_pipe), n_pipe)

    slots = {}
    sources = {}

    def copy_of(name, src, dst, device):
        k = slots.setdefault(name, len(slots))
        return pltpu.make_async_remote_copy(
            src_ref=src,
            dst_ref=dst,
            send_sem=send_sem.at[k],
            recv_sem=recv_sem.at[k],
            device_id=device,
            device_id_type=MESH,
        )

    def send(name, src, device, dst=None):
        sources[name] = src
        copy_of(name, src(), src() if dst is None else dst(), device).start()

    def land(name, dst):
        copy_of(name, dst, dst, (p, y, x)).wait_recv()

    load_w = pltpu.make_async_copy(wi_hbm, wloc, local_sem.at[0])
    load_x = pltpu.make_async_copy(x_hbm, xg.at[0], local_sem.at[1])
    own_cols = pl.ds(pl.multiple_of(x * out_cols, out_cols), out_cols)
    load_o = pltpu.make_async_copy(
        wo_hbm.at[:, own_cols], wo.at[y, x], local_sem.at[2]
    )
    load_g = pltpu.make_async_copy(gain_hbm, gain, local_sem.at[3])
    load_l = pltpu.make_async_copy(lengths_hbm, lengths, local_sem.at[4])
    load_w.start()
    load_x.start()

    barrier = pltpu.get_barrier_semaphore()
    peers = [(p, y, xs(d)) for d in (1, 2, 3)]
    peers += [(p, ys(d), x) for d in (1, -1)]
    peers += [(p, ys(-2), x)]
    for peer in peers + [(ps(-1), y, xs(d)) for d in range(NX)]:
        pl.semaphore_signal(barrier, inc=1, device_id=peer, device_id_type=MESH)
    load_l.start()
    load_g.start()
    load_o.start()

    load_w.wait()
    w_rows = wloc.shape[0]
    lane_w = lax.broadcasted_iota(jnp.int32, (w_rows, 128), 1)
    q_width = HEADS * HEAD_DIM
    g_width = GROUP * HEAD_DIM
    for t in range(NX):
        k_tile = wloc[:, q_width + 128 * (t // 2) : q_width + 128 * (t // 2) + 128]
        v_at = q_width + KV_HEADS * HEAD_DIM + 128 * (t // 2)
        v_tile = wloc[:, v_at : v_at + 128]
        k_tile = k_tile.astype(jnp.float32)
        v_tile = v_tile.astype(jnp.float32)
        if t % 2 == 0:
            v_tile = pltpu.roll(v_tile, 64, 1)
        else:
            k_tile = pltpu.roll(k_tile, 64, 1)
        wsp[t] = jnp.where(lane_w < 64, k_tile, v_tile).astype(jnp.bfloat16)

    def q_cols(d):
        return pl.ds(pl.multiple_of(xs(d) * g_width, g_width), g_width)

    wkv[y, x] = wsp[x]
    wq[y, x] = wloc[:, q_cols(0)]
    load_x.wait()
    with jax.named_scope("barrier"):
        pl.semaphore_wait(barrier, len(peers) + NX)

    north, south = (p, ys(1), x), (p, ys(-1), x)
    up, down = (p, y, xs(1)), (p, y, xs(-1))
    toward = {1: north, -1: south}
    reach = n_y // 2
    order = ((0, 1), (0, -1), (-1, 1), (-1, -1), (1, 1), (1, -1), (2, 1), (2, -1))
    only_south = ((0, -1), (-1, -1), (1, -1), (2, -1))
    rings = {"kv": (wkv, only_south), "q": (wq, only_south), "o": (wo, only_south)}

    def ring_send(ring, d, way, step):
        buf = rings[ring][0]
        send(
            (ring, d, way, step),
            lambda: buf.at[ys(-way * step), xs(d)],
            toward[way],
        )

    def ring_step(ring, step, pieces=order):
        buf, final = rings[ring]
        if not 0 <= step < reach:
            return
        with jax.named_scope(f"{ring}_ring{step}"):
            for d, way in pieces:
                if step == reach - 1 and (d, way) not in final:
                    continue
                land((ring, d, way, step), buf.at[ys(-way * (step + 1)), xs(d)])
                if step + 1 < reach - 1 or (step + 1 == reach - 1 and (d, way) in final):
                    ring_send(ring, d, way, step + 1)

    def ring_steps(ring, *steps):
        for step in steps:
            if 0 <= step < reach - 1:
                ring_step(ring, step)

    def ring_own(ring):
        for way in (1, -1):
            ring_send(ring, 0, way, 0)

    def exchange(ring, source):
        buf = rings[ring][0]
        for d in (1, -1, 2):
            send((ring, d), lambda d=d: source(d), (p, y, xs(d)), lambda: buf.at[y, x])

    def ring_join(ring, *ways):
        with jax.named_scope(f"{ring}_join"):
            for d in (1, -1, 2):
                land((ring, d), rings[ring][0].at[y, xs(-d)])
                e = d if d == 2 else -d
                for way in ways:
                    ring_send(ring, e, way, 0)

    first, second = pl.ds(0, half), pl.ds(half, half)

    def x_start():
        send("x_up_a", lambda: xg.at[0, first], up, lambda: xg.at[1, first])
        send("x_down_b", lambda: xg.at[0, second], down, lambda: xg.at[2, second])
        send("x_up_b", lambda: xg.at[0, second], up, lambda: xg.at[1, second])
        send("x_down_a", lambda: xg.at[0, first], down, lambda: xg.at[2, first])

    def x_pass():
        with jax.named_scope("x_first"):
            land("x_up_a", xg.at[1, first])
            send("x_far_a", lambda: xg.at[1, first], up, lambda: xg.at[3, first])
            land("x_down_b", xg.at[2, second])
            send("x_far_b", lambda: xg.at[2, second], down, lambda: xg.at[3, second])

    def x_second():
        with jax.named_scope("x_second"):
            land("x_up_b", xg.at[1, second])
            land("x_down_a", xg.at[2, first])

    def x_far():
        with jax.named_scope("x_far"):
            land("x_far_a", xg.at[3, first])
            land("x_far_b", xg.at[3, second])

    def kv_exchange():
        exchange("kv", lambda d: wsp.at[xs(d)])

    def q_exchange():
        exchange("q", lambda d: wloc.at[:, q_cols(d)])

    def o_exchange():
        exchange("o", lambda d: wo_hbm.at[:, o_cols(d)])

    def o_cols(d):
        return pl.ds(pl.multiple_of(xs(d) * out_cols, out_cols), out_cols)

    load_l.wait()
    load_g.wait()
    ends = []
    total = 0
    for i in range(lengths.shape[0]):
        total = total + lengths[i, p]
        ends.append(total)
    deltas = (0, -1, 1, 2)
    lane = lax.broadcasted_iota(jnp.int32, (rows, 128), 1)
    row = lax.broadcasted_iota(jnp.int32, (rows, 128), 0)
    half_dim = HEAD_DIM // 2
    turn = lax.broadcasted_iota(jnp.int32, (8, 128), 1) & (half_dim - 1)
    inverse = jnp.zeros((8, 128), jnp.float32)
    for i in range(half_dim):
        inverse = jnp.where(turn == i, rope_base ** (-2.0 * i / HEAD_DIM), inverse)

    def make_trig(slot):
        spots = y * span + xs(deltas[slot]) * rows + row
        place_in = (spots - response_start(ends, spots)).astype(jnp.float32)
        sine, cosine = sine_cosine(place_in * inverse[:1])
        trig[slot, 0] = cosine
        trig[slot, 1] = jnp.where((lane & 63) < 32, -sine, sine)

    norm_rows = 32

    def normalize(slot):
        def step(i, carry):
            at = pl.ds(pl.multiple_of(i * norm_rows, norm_rows), norm_rows)
            wide = xg[slot, at, :].astype(jnp.float32)
            scale = lax.rsqrt(jnp.mean(wide * wide, -1, keepdims=True) + epsilon)
            to = pl.ds(pl.multiple_of(slot * rows + i * norm_rows, norm_rows), norm_rows)
            xn[to, :] = (wide * scale * gain[...]).astype(jnp.bfloat16)
            return carry

        lax.fori_loop(0, rows // norm_rows, step, 0, unroll=2)

    def rotated(tile, slot):
        partner = jnp.where((lane & 63) < 32, pltpu.roll(tile, 96, 1), pltpu.roll(tile, 32, 1))
        return tile * trig[slot, 0] + partner * trig[slot, 1]

    def project(slot, count, buf):
        return jnp.dot(
            xn[slot * rows : (slot + count) * rows, :],
            buf[...].reshape(depth, buf.shape[3]),
            preferred_element_type=jnp.float32,
        )

    def own_kv(slot):
        return kv.at[2 * NX + xs(deltas[slot])]

    def near_kv(slot):
        return kv.at[NX + xs(deltas[slot])]

    def far_kv(slot):
        return kv.at[xs(deltas[slot])]

    def project_kv(slot, count):
        with jax.named_scope(f"kv{slot}"):
            proj = project(slot, count, wkv)
            for i in range(count):
                own = proj[i * rows : (i + 1) * rows]
                own = jnp.where(lane < 64, rotated(own, slot + i), own)
                kv[2 * NX + xs(deltas[slot + i])] = own.astype(jnp.bfloat16)
                if slot + i == 3:
                    send(
                        ("far", 3),
                        lambda: own_kv(3),
                        (p, ys(2), x),
                        lambda: far_kv(3),
                    )
                send(
                    ("near", slot + i),
                    lambda i=i: own_kv(slot + i),
                    north,
                    lambda i=i: near_kv(slot + i),
                )

    def kv_pass():
        with jax.named_scope("kv_pass"):
            for slot in range(3):
                land(("near", slot), near_kv(slot))
                send(("far", slot), lambda slot=slot: near_kv(slot), north, lambda: far_kv(slot))

    def project_q(slot, count):
        proj = project(slot, count, wq)
        for i in range(count):
            own = proj[i * rows : (i + 1) * rows]
            block = xs(deltas[slot + i])
            for t in range(GROUP // 2):
                tile = rotated(own[:, 128 * t : 128 * (t + 1)], slot + i) * HEAD_DIM**-0.5
                q_s[block, 2 * t] = jnp.where(lane < 64, tile, 0.0).astype(jnp.bfloat16)
                q_s[block, 2 * t + 1] = jnp.where(
                    lane < 64, pltpu.roll(tile, 64, 1), 0.0
                ).astype(jnp.bfloat16)

    lane_p = lax.broadcasted_iota(jnp.int32, (part, 128), 1)
    row_p = lax.broadcasted_iota(jnp.int32, (part, 128), 0)

    def make_masks(i):
        def one(j, carry):
            spots = y * span + j * rows + i * part + row_p
            start = response_start(ends, spots)
            for c in range(WINDOW):
                keys = y * span + (j + c - 2 * NX) * rows + lane_p
                inside = keys >= start
                if c == WINDOW - 1:
                    inside = inside & (keys <= spots)
                masks[i, j, :, c * rows : (c + 1) * rows] = jnp.where(inside, 0.0, masked_score)
            return carry

        lax.fori_loop(0, NX, one, 0)

    def prepare():
        with jax.named_scope("trig"):
            for slot in range(4):
                make_trig(slot)
        with jax.named_scope("norm0"):
            normalize(0)
        with jax.named_scope("masks"):
            for i in range(CHUNKS):
                make_masks(i)

    def norms(*which):
        with jax.named_scope("norms"):
            for slot in which:
                normalize(slot)

    def last_block():
        x_far()
        norms(3)
        project_kv(3, 1)

    def queries_of(slot, count):
        with jax.named_scope(f"q{slot}"):
            project_q(slot, count)

    late = lax.rem(p + p // (n_pipe - 2), 2) == 1
    ring_own("kv")
    kv_exchange()
    ring_own("q")
    q_exchange()

    @pl.when(jnp.logical_not(late))
    def _():
        x_start()

    prepare()
    ring_join("kv", 1, -1)

    later = jnp.logical_or(p == n_pipe - 2, p == 1)

    @pl.when(jnp.logical_and(late, jnp.logical_not(later)))
    def _():
        x_start()

    ring_join("q", 1, -1)

    @pl.when(later)
    def _():
        x_start()

    ring_steps("kv", 0)
    ring_steps("q", 0)
    ring_steps("kv", 1)
    x_pass()
    o_exchange()
    ring_steps("kv", *range(2, reach))
    ring_steps("q", 1)
    ring_step("kv", reach - 1)
    x_second()
    norms(1, 2)
    project_kv(0, 3)
    ring_steps("q", *range(2, reach))
    last_block()
    going_north = ((-1, 1), (1, 1), (2, 1))
    going_south = ((-1, -1), (1, -1), (2, -1))
    load_o.wait()
    kv_pass()
    ring_send("o", 0, -1, 0)
    ring_join("o", -1)
    ring_step("q", reach - 1)
    queries_of(0, 3)
    queries_of(3, 1)
    with jax.named_scope("kv_near"):
        land(("near", 3), near_kv(3))
    for d in (0, -1, 1, 2):
        ring_send("o", d, 1, 0)
    with jax.named_scope("kv_far"):
        for slot in range(4):
            land(("far", slot), far_kv(slot))
    with jax.named_scope("v_one"):
        for b in range(3 * NX):
            v_one[b] = jnp.where(lane < 64, 1.0, kv[b].astype(jnp.float32)).astype(jnp.bfloat16)

    def attend(i, j):
        queries = q_s[j, :, i * part : (i + 1) * part, :].reshape(GROUP * part, 128)
        window = kv[j : j + WINDOW].reshape(WINDOW * rows, 128)
        values = v_one[j : j + WINDOW].reshape(WINDOW * rows, 128)
        scores = lax.dot_general(
            queries, window, (((1,), (1,)), ((), ())), preferred_element_type=jnp.float32
        )
        scores = scores.reshape(GROUP, part, WINDOW * rows) + masks[i, j][None]
        probs = jnp.exp(scores - jnp.max(scores, -1, keepdims=True))
        mixed = jnp.dot(
            probs.astype(jnp.bfloat16).reshape(GROUP * part, WINDOW * rows),
            values,
            preferred_element_type=jnp.float32,
        )
        turned = pltpu.roll(mixed, 64, 1)
        tiles = []
        for t in range(GROUP // 2):
            even = slice(2 * t * part, (2 * t + 1) * part)
            odd = slice((2 * t + 1) * part, (2 * t + 2) * part)
            tiles.append(
                jnp.where(lane_p < 64, turned[even] / mixed[even], mixed[odd] / turned[odd])
            )
        att[i, x, j] = jnp.concatenate(tiles, 1).astype(jnp.bfloat16)

    low, high = pl.ds(0, NX // 2), pl.ds(NX // 2, NX // 2)

    def piece(i, d, which):
        return att.at[i, xs(d), which]

    def att_start(i):
        send(("up_l", i), lambda: piece(i, 0, low), up)
        send(("down_h", i), lambda: piece(i, 0, high), down)
        send(("up_h", i), lambda: piece(i, 0, high), up)
        send(("down_l", i), lambda: piece(i, 0, low), down)

    def att_pass(i):
        with jax.named_scope(f"pass{i}"):
            land(("up_l", i), piece(i, -1, low))
            send(("far_l", i), lambda: piece(i, -1, low), up)
            land(("down_h", i), piece(i, 1, high))
            send(("far_h", i), lambda: piece(i, 1, high), down)

    def att_in(i):
        with jax.named_scope(f"att{i}_in"):
            land(("up_h", i), piece(i, -1, high))
            land(("down_l", i), piece(i, 1, low))
            land(("far_l", i), piece(i, 2, low))
            land(("far_h", i), piece(i, 2, high))

    def out_part(i, d):
        return out.at[pl.ds(i * part, part), o_cols(d)]

    def finish(i):
        weight = wo[...].reshape(q_width, out_cols)
        result = None
        for h in range(NX):
            term = jnp.dot(
                att[i, h].reshape(NX * part, g_width),
                weight[h * g_width : (h + 1) * g_width],
                preferred_element_type=jnp.float32,
            )
            result = term if result is None else result + term
        acc[...] = result
        for slot in (3, 2, 1, 0):
            j = xs(deltas[slot])
            kept = xg[slot, i * part : (i + 1) * part, own_cols].astype(jnp.float32)
            at = pl.ds(pl.multiple_of(j * part, part), part)
            obuf[i, slot] = (acc[at, :] + kept).astype(jnp.bfloat16)
            send(
                ("out", i, slot),
                lambda slot=slot: obuf.at[i, slot],
                (ps(1), y, j),
                lambda: out_part(i, 0),
            )

    def o_steps(step, pieces):
        if step < reach - 1:
            ring_step("o", step, pieces)

    attend(0, 0)
    ring_step("o", 0, ((0, -1),) + going_south)
    attend(0, 1)
    with jax.named_scope("attend0b"):
        attend(0, 2)
        attend(0, 3)
    att_start(0)
    with jax.named_scope("attend1a"):
        attend(1, 0)
        attend(1, 1)
    ring_step("o", 0, ((0, 1),) + going_north)
    o_steps(1, ((0, -1),) + going_south)
    with jax.named_scope("attend1b"):
        attend(1, 2)
        attend(1, 3)
    att_pass(0)
    att_start(1)
    o_steps(1, ((0, 1),) + going_north)
    for step in range(2, reach - 1):
        o_steps(step, ((0, -1),) + going_south)
    att_in(0)
    att_pass(1)
    for step in range(2, reach - 1):
        o_steps(step, ((0, 1),) + going_north)
    ring_step("o", reach - 1)
    with jax.named_scope("finish0"):
        finish(0)
    att_in(1)
    with jax.named_scope("finish1"):
        finish(1)
    with jax.named_scope("out_in"):
        for i in range(CHUNKS):
            for slot in (3, 2, 1, 0):
                land(("out", i, slot), out_part(i, -deltas[slot]))
    with jax.named_scope("wait_send"):
        for name, src in sources.items():
            copy_of(name, src(), src(), (p, y, x)).wait_send()


def body(states, norm_gain, w_in, w_out, lengths):
    rows, depth = states.shape[1:]
    w_rows = w_in.shape[1]
    o_rows = w_out.shape[1]
    out_cols = depth // NX
    n_pipe = lax.axis_size("pipe")
    n_y = lax.axis_size("ctx_y")
    part = rows // CHUNKS
    copies = 160
    bf16, f32 = jnp.bfloat16, jnp.float32
    moved = pl.pallas_call(
        functools.partial(tick_kernel, n_pipe, n_y),
        out_shape=pltpu.VMEM((rows, depth), bf16),
        in_specs=[
            pl.BlockSpec(memory_space=pl.ANY),
            pl.BlockSpec(memory_space=pl.ANY),
            pl.BlockSpec(memory_space=pl.ANY),
            pl.BlockSpec(memory_space=pl.ANY),
            pl.BlockSpec(memory_space=pl.ANY),
        ],
        out_specs=pl.BlockSpec(memory_space=pltpu.VMEM),
        scratch_shapes=[
            pltpu.SMEM(lengths.shape[::-1], jnp.int32),
            pltpu.VMEM((1, depth), f32),
            pltpu.VMEM((4, rows, depth), bf16),
            pltpu.VMEM((4 * rows, depth), bf16),
            pltpu.VMEM((w_rows, w_in.shape[2]), bf16),
            pltpu.VMEM((NX, w_rows, 128), bf16),
            pltpu.VMEM((n_y, NX, w_rows, 128), bf16),
            pltpu.VMEM((n_y, NX, w_rows, GROUP * HEAD_DIM), bf16),
            pltpu.VMEM((n_y, NX, o_rows, out_cols), bf16),
            pltpu.VMEM((4, 2, rows, 128), f32),
            pltpu.VMEM((CHUNKS, NX, part, WINDOW * rows), f32),
            pltpu.VMEM((NX, GROUP, rows, 128), bf16),
            pltpu.VMEM((3 * NX, rows, 128), bf16),
            pltpu.VMEM((3 * NX, rows, 128), bf16),
            pltpu.VMEM((CHUNKS, NX, NX, part, GROUP * HEAD_DIM), bf16),
            pltpu.VMEM((NX * part, out_cols), f32),
            pltpu.VMEM((CHUNKS, 4, part, out_cols), bf16),
            pltpu.SemaphoreType.DMA((5,)),
            pltpu.SemaphoreType.DMA((copies,)),
            pltpu.SemaphoreType.DMA((copies,)),
        ],
        compiler_params=pltpu.CompilerParams(
            collective_id=0, has_side_effects=True, vmem_limit_bytes=60 * 1024 * 1024
        ),
        name="tick",
    )(lengths.T, norm_gain, states[0], w_in[0], w_out[0])
    return moved[None]


def solution(mesh):
    n_pipe = mesh.shape["pipe"]
    n_y = mesh.shape["ctx"] // NX
    finer = Mesh(mesh.devices.reshape(n_pipe, n_y, NX), ("pipe", "ctx_y", "ctx_x"))
    ctx = ("ctx_y", "ctx_x")
    placed = (
        P("pipe", ctx, None),
        P("pipe", None),
        P("pipe", ctx, None),
        P("pipe", ctx, None),
        P(),
    )
    return jax.shard_map(
        body, mesh=finer, in_specs=placed, out_specs=P("pipe", ctx, None), check_vma=False
    )
```

```python
import functools
import math

import jax
import jax.numpy as jnp
from jax import lax
from jax.experimental import pallas as pl
from jax.experimental.pallas import tpu as pltpu
from jax.sharding import Mesh
from jax.sharding import PartitionSpec as P

HEAD_DIM = 64
HEADS = 16
KV_HEADS = 4
GROUP = HEADS // KV_HEADS
NX = 4
CHUNKS = 2
WINDOW = 9

epsilon = 1e-05
rope_base = 500000.0
masked_score = -1e30
MESH = pl.DeviceIdType.MESH


def sine_cosine(angle):
    turns = jnp.floor(angle * (2.0 / math.pi) + 0.5)
    quarter = turns.astype(jnp.int32)
    rest = angle - turns * 1.5703125
    rest = rest - turns * 4.837512969970703125e-4
    rest = rest - turns * 7.54978995489188216e-8
    z = rest * rest
    sine = ((-1.9515295891e-4 * z + 8.3321608736e-3) * z - 1.6666654611e-1) * z * rest + rest
    cosine = (
        (2.443315711809948e-5 * z - 1.388731625493765e-3) * z + 4.166664568298827e-2
    ) * z * z - 0.5 * z + 1.0
    odd = (quarter & 1) == 1
    sine, cosine = jnp.where(odd, cosine, sine), jnp.where(odd, sine, cosine)
    sine = jnp.where((quarter & 2) == 2, -sine, sine)
    cosine = jnp.where(((quarter + 1) & 2) == 2, -cosine, cosine)
    return sine, cosine


def response_start(ends, spots):
    start = jnp.zeros_like(spots)
    for end in ends:
        start = jnp.maximum(start, jnp.where(spots >= end, end, 0))
    return start


def tick_kernel(
    n_pipe,
    n_y,
    lengths_hbm,
    gain_hbm,
    x_hbm,
    wi_hbm,
    wo_hbm,
    out,
    lengths,
    gain,
    xg,
    xn,
    wloc,
    wsp,
    wkv,
    wq,
    wo,
    trig,
    masks,
    q_s,
    kv,
    v_one,
    att,
    acc,
    obuf,
    local_sem,
    send_sem,
    recv_sem,
):
    p = lax.axis_index("pipe")
    y = lax.axis_index("ctx_y")
    x = lax.axis_index("ctx_x")
    rows = xg.shape[1]
    half = rows // 2
    part = rows // CHUNKS
    depth = xg.shape[2]
    out_cols = acc.shape[1]
    span = NX * rows

    def xs(d):
        return lax.rem(x + (d + NX), NX)

    def ys(d):
        return lax.rem(y + (d + n_y), n_y)

    def ps(d):
        return lax.rem(p + (d + n_pipe), n_pipe)

    slots = {}
    sources = {}

    def copy_of(name, src, dst, device):
        k = slots.setdefault(name, len(slots))
        return pltpu.make_async_remote_copy(
            src_ref=src,
            dst_ref=dst,
            send_sem=send_sem.at[k],
            recv_sem=recv_sem.at[k],
            device_id=device,
            device_id_type=MESH,
        )

    def send(name, src, device, dst=None):
        sources[name] = src
        copy_of(name, src(), src() if dst is None else dst(), device).start()

    def land(name, dst):
        copy_of(name, dst, dst, (p, y, x)).wait_recv()

    load_w = pltpu.make_async_copy(wi_hbm, wloc, local_sem.at[0])
    load_x = pltpu.make_async_copy(x_hbm, xg.at[0], local_sem.at[1])
    own_cols = pl.ds(pl.multiple_of(x * out_cols, out_cols), out_cols)
    load_o = pltpu.make_async_copy(
        wo_hbm.at[:, own_cols], wo.at[y, x], local_sem.at[2]
    )
    load_g = pltpu.make_async_copy(gain_hbm, gain, local_sem.at[3])
    load_l = pltpu.make_async_copy(lengths_hbm, lengths, local_sem.at[4])
    load_w.start()
    load_x.start()

    barrier = pltpu.get_barrier_semaphore()
    peers = [(p, y, xs(d)) for d in (1, 2, 3)]
    peers += [(p, ys(d), x) for d in (1, -1)]
    peers += [(p, ys(-2), x)]
    for peer in peers + [(ps(-1), y, xs(d)) for d in range(NX)]:
        pl.semaphore_signal(barrier, inc=1, device_id=peer, device_id_type=MESH)
    load_l.start()
    load_g.start()
    load_o.start()

    load_w.wait()
    w_rows = wloc.shape[0]
    lane_w = lax.broadcasted_iota(jnp.int32, (w_rows, 128), 1)
    q_width = HEADS * HEAD_DIM
    g_width = GROUP * HEAD_DIM
    for t in range(NX):
        k_tile = wloc[:, q_width + 128 * (t // 2) : q_width + 128 * (t // 2) + 128]
        v_at = q_width + KV_HEADS * HEAD_DIM + 128 * (t // 2)
        v_tile = wloc[:, v_at : v_at + 128]
        k_tile = k_tile.astype(jnp.float32)
        v_tile = v_tile.astype(jnp.float32)
        if t % 2 == 0:
            v_tile = pltpu.roll(v_tile, 64, 1)
        else:
            k_tile = pltpu.roll(k_tile, 64, 1)
        wsp[t] = jnp.where(lane_w < 64, k_tile, v_tile).astype(jnp.bfloat16)

    def q_cols(d):
        return pl.ds(pl.multiple_of(xs(d) * g_width, g_width), g_width)

    wkv[y, x] = wsp[x]
    wq[y, x] = wloc[:, q_cols(0)]
    load_x.wait()
    with jax.named_scope("barrier"):
        pl.semaphore_wait(barrier, len(peers) + NX)

    north, south = (p, ys(1), x), (p, ys(-1), x)
    up, down = (p, y, xs(1)), (p, y, xs(-1))
    toward = {1: north, -1: south}
    reach = n_y // 2
    order = ((0, 1), (0, -1), (-1, 1), (-1, -1), (1, 1), (1, -1), (2, 1), (2, -1))
    only_south = ((0, -1), (-1, -1), (1, -1), (2, -1))
    rings = {"kv": (wkv, only_south), "q": (wq, only_south), "o": (wo, only_south)}

    def ring_send(ring, d, way, step):
        buf = rings[ring][0]
        send(
            (ring, d, way, step),
            lambda: buf.at[ys(-way * step), xs(d)],
            toward[way],
        )

    def ring_step(ring, step, pieces=order):
        buf, final = rings[ring]
        if not 0 <= step < reach:
            return
        with jax.named_scope(f"{ring}_ring{step}"):
            for d, way in pieces:
                if step == reach - 1 and (d, way) not in final:
                    continue
                land((ring, d, way, step), buf.at[ys(-way * (step + 1)), xs(d)])
                if step + 1 < reach - 1 or (step + 1 == reach - 1 and (d, way) in final):
                    ring_send(ring, d, way, step + 1)

    def ring_steps(ring, *steps):
        for step in steps:
            if 0 <= step < reach - 1:
                ring_step(ring, step)

    def ring_own(ring):
        for way in (1, -1):
            ring_send(ring, 0, way, 0)

    def exchange(ring, source):
        buf = rings[ring][0]
        for d in (1, -1, 2):
            send((ring, d), lambda d=d: source(d), (p, y, xs(d)), lambda: buf.at[y, x])

    def ring_join(ring, *ways):
        with jax.named_scope(f"{ring}_join"):
            for d in (1, -1, 2):
                land((ring, d), rings[ring][0].at[y, xs(-d)])
                e = d if d == 2 else -d
                for way in ways:
                    ring_send(ring, e, way, 0)

    first, second = pl.ds(0, half), pl.ds(half, half)

    def x_start():
        send("x_up_a", lambda: xg.at[0, first], up, lambda: xg.at[1, first])
        send("x_down_b", lambda: xg.at[0, second], down, lambda: xg.at[2, second])
        send("x_up_b", lambda: xg.at[0, second], up, lambda: xg.at[1, second])
        send("x_down_a", lambda: xg.at[0, first], down, lambda: xg.at[2, first])

    def x_pass():
        with jax.named_scope("x_first"):
            land("x_up_a", xg.at[1, first])
            send("x_far_a", lambda: xg.at[1, first], up, lambda: xg.at[3, first])
            land("x_down_b", xg.at[2, second])
            send("x_far_b", lambda: xg.at[2, second], down, lambda: xg.at[3, second])

    def x_second():
        with jax.named_scope("x_second"):
            land("x_up_b", xg.at[1, second])
            land("x_down_a", xg.at[2, first])

    def x_far():
        with jax.named_scope("x_far"):
            land("x_far_a", xg.at[3, first])
            land("x_far_b", xg.at[3, second])

    def kv_exchange():
        exchange("kv", lambda d: wsp.at[xs(d)])

    def q_exchange():
        exchange("q", lambda d: wloc.at[:, q_cols(d)])

    def o_exchange():
        exchange("o", lambda d: wo_hbm.at[:, o_cols(d)])

    def o_cols(d):
        return pl.ds(pl.multiple_of(xs(d) * out_cols, out_cols), out_cols)

    load_l.wait()
    load_g.wait()
    ends = []
    total = 0
    for i in range(lengths.shape[0]):
        total = total + lengths[i, p]
        ends.append(total)
    deltas = (0, -1, 1, 2)
    lane = lax.broadcasted_iota(jnp.int32, (rows, 128), 1)
    row = lax.broadcasted_iota(jnp.int32, (rows, 128), 0)
    half_dim = HEAD_DIM // 2
    turn = lax.broadcasted_iota(jnp.int32, (8, 128), 1) & (half_dim - 1)
    inverse = jnp.zeros((8, 128), jnp.float32)
    for i in range(half_dim):
        inverse = jnp.where(turn == i, rope_base ** (-2.0 * i / HEAD_DIM), inverse)

    def make_trig(slot):
        spots = y * span + xs(deltas[slot]) * rows + row
        place_in = (spots - response_start(ends, spots)).astype(jnp.float32)
        sine, cosine = sine_cosine(place_in * inverse[:1])
        trig[slot, 0] = cosine
        trig[slot, 1] = jnp.where((lane & 63) < 32, -sine, sine)

    norm_rows = 32

    def normalize(slot):
        def step(i, carry):
            at = pl.ds(pl.multiple_of(i * norm_rows, norm_rows), norm_rows)
            wide = xg[slot, at, :].astype(jnp.float32)
            scale = lax.rsqrt(jnp.mean(wide * wide, -1, keepdims=True) + epsilon)
            to = pl.ds(pl.multiple_of(slot * rows + i * norm_rows, norm_rows), norm_rows)
            xn[to, :] = (wide * scale * gain[...]).astype(jnp.bfloat16)
            return carry

        lax.fori_loop(0, rows // norm_rows, step, 0, unroll=2)

    def rotated(tile, slot):
        partner = jnp.where((lane & 63) < 32, pltpu.roll(tile, 96, 1), pltpu.roll(tile, 32, 1))
        return tile * trig[slot, 0] + partner * trig[slot, 1]

    def project(slot, count, buf):
        return jnp.dot(
            xn[slot * rows : (slot + count) * rows, :],
            buf[...].reshape(depth, buf.shape[3]),
            preferred_element_type=jnp.float32,
        )

    def own_kv(slot):
        return kv.at[2 * NX + xs(deltas[slot])]

    def near_kv(slot):
        return kv.at[NX + xs(deltas[slot])]

    def far_kv(slot):
        return kv.at[xs(deltas[slot])]

    def project_kv(slot, count):
        with jax.named_scope(f"kv{slot}"):
            proj = project(slot, count, wkv)
            for i in range(count):
                own = proj[i * rows : (i + 1) * rows]
                own = jnp.where(lane < 64, rotated(own, slot + i), own)
                kv[2 * NX + xs(deltas[slot + i])] = own.astype(jnp.bfloat16)
                if slot + i == 3:
                    send(
                        ("far", 3),
                        lambda: own_kv(3),
                        (p, ys(2), x),
                        lambda: far_kv(3),
                    )
                send(
                    ("near", slot + i),
                    lambda i=i: own_kv(slot + i),
                    north,
                    lambda i=i: near_kv(slot + i),
                )

    def kv_pass():
        with jax.named_scope("kv_pass"):
            for slot in range(3):
                land(("near", slot), near_kv(slot))
                send(("far", slot), lambda slot=slot: near_kv(slot), north, lambda: far_kv(slot))

    def project_q(slot, count):
        proj = project(slot, count, wq)
        for i in range(count):
            own = proj[i * rows : (i + 1) * rows]
            block = xs(deltas[slot + i])
            for t in range(GROUP // 2):
                tile = rotated(own[:, 128 * t : 128 * (t + 1)], slot + i) * HEAD_DIM**-0.5
                q_s[block, 2 * t] = jnp.where(lane < 64, tile, 0.0).astype(jnp.bfloat16)
                q_s[block, 2 * t + 1] = jnp.where(
                    lane < 64, pltpu.roll(tile, 64, 1), 0.0
                ).astype(jnp.bfloat16)

    lane_p = lax.broadcasted_iota(jnp.int32, (part, 128), 1)
    row_p = lax.broadcasted_iota(jnp.int32, (part, 128), 0)

    def make_masks(i):
        def one(j, carry):
            spots = y * span + j * rows + i * part + row_p
            start = response_start(ends, spots)
            for c in range(WINDOW):
                keys = y * span + (j + c - 2 * NX) * rows + lane_p
                inside = keys >= start
                if c == WINDOW - 1:
                    inside = inside & (keys <= spots)
                masks[i, j, :, c * rows : (c + 1) * rows] = jnp.where(inside, 0.0, masked_score)
            return carry

        lax.fori_loop(0, NX, one, 0)

    def prepare():
        with jax.named_scope("trig"):
            for slot in range(4):
                make_trig(slot)
        with jax.named_scope("norm0"):
            normalize(0)
        with jax.named_scope("masks"):
            for i in range(CHUNKS):
                make_masks(i)

    def norms(*which):
        with jax.named_scope("norms"):
            for slot in which:
                normalize(slot)

    def last_block():
        x_far()
        norms(3)
        project_kv(3, 1)

    def queries_of(slot, count):
        with jax.named_scope(f"q{slot}"):
            project_q(slot, count)

    late = lax.rem(p + p // (n_pipe - 2), 2) == 1
    ring_own("kv")
    kv_exchange()
    ring_own("q")
    q_exchange()

    @pl.when(jnp.logical_not(late))
    def _():
        x_start()

    prepare()
    ring_join("kv", 1, -1)

    later = jnp.logical_or(p == n_pipe - 2, p == 1)

    @pl.when(jnp.logical_and(late, jnp.logical_not(later)))
    def _():
        x_start()

    ring_join("q", 1, -1)

    @pl.when(later)
    def _():
        x_start()

    ring_steps("kv", 0)
    ring_steps("q", 0)
    ring_steps("kv", 1)
    x_pass()
    o_exchange()
    ring_steps("kv", *range(2, reach))
    ring_steps("q", 1)
    ring_step("kv", reach - 1)
    x_second()
    norms(1, 2)
    project_kv(0, 3)
    ring_steps("q", *range(2, reach))
    last_block()
    going_north = ((-1, 1), (1, 1), (2, 1))
    going_south = ((-1, -1), (1, -1), (2, -1))
    load_o.wait()
    kv_pass()
    ring_send("o", 0, -1, 0)
    ring_join("o", -1)
    ring_step("q", reach - 1)
    queries_of(0, 3)
    queries_of(3, 1)
    with jax.named_scope("kv_near"):
        land(("near", 3), near_kv(3))
    for d in (0, -1, 1, 2):
        ring_send("o", d, 1, 0)
    with jax.named_scope("kv_far"):
        for slot in range(4):
            land(("far", slot), far_kv(slot))
    with jax.named_scope("v_one"):
        for b in range(3 * NX):
            v_one[b] = jnp.where(lane < 64, 1.0, kv[b].astype(jnp.float32)).astype(jnp.bfloat16)

    def attend(i, j):
        queries = q_s[j, :, i * part : (i + 1) * part, :].reshape(GROUP * part, 128)
        window = kv[j : j + WINDOW].reshape(WINDOW * rows, 128)
        values = v_one[j : j + WINDOW].reshape(WINDOW * rows, 128)
        scores = lax.dot_general(
            queries, window, (((1,), (1,)), ((), ())), preferred_element_type=jnp.float32
        )
        scores = scores.reshape(GROUP, part, WINDOW * rows) + masks[i, j][None]
        probs = jnp.exp(scores - jnp.max(scores, -1, keepdims=True))
        mixed = jnp.dot(
            probs.astype(jnp.bfloat16).reshape(GROUP * part, WINDOW * rows),
            values,
            preferred_element_type=jnp.float32,
        )
        turned = pltpu.roll(mixed, 64, 1)
        tiles = []
        for t in range(GROUP // 2):
            even = slice(2 * t * part, (2 * t + 1) * part)
            odd = slice((2 * t + 1) * part, (2 * t + 2) * part)
            tiles.append(
                jnp.where(lane_p < 64, turned[even] / mixed[even], mixed[odd] / turned[odd])
            )
        att[i, x, j] = jnp.concatenate(tiles, 1).astype(jnp.bfloat16)

    low, high = pl.ds(0, NX // 2), pl.ds(NX // 2, NX // 2)

    def piece(i, d, which):
        return att.at[i, xs(d), which]

    def att_low(i):
        send(("up_l", i), lambda: piece(i, 0, low), up)
        send(("down_l", i), lambda: piece(i, 0, low), down)

    def att_high(i):
        send(("down_h", i), lambda: piece(i, 0, high), down)
        send(("up_h", i), lambda: piece(i, 0, high), up)

    def att_start(i):
        send(("up_l", i), lambda: piece(i, 0, low), up)
        send(("down_h", i), lambda: piece(i, 0, high), down)
        send(("up_h", i), lambda: piece(i, 0, high), up)
        send(("down_l", i), lambda: piece(i, 0, low), down)

    def att_pass(i):
        with jax.named_scope(f"pass{i}"):
            land(("up_l", i), piece(i, -1, low))
            send(("far_l", i), lambda: piece(i, -1, low), up)
            land(("down_h", i), piece(i, 1, high))
            send(("far_h", i), lambda: piece(i, 1, high), down)

    def att_in(i):
        with jax.named_scope(f"att{i}_in"):
            land(("up_h", i), piece(i, -1, high))
            land(("down_l", i), piece(i, 1, low))
            land(("far_l", i), piece(i, 2, low))
            land(("far_h", i), piece(i, 2, high))

    def out_part(i, d):
        return out.at[pl.ds(i * part, part), o_cols(d)]

    def finish(i):
        weight = wo[...].reshape(q_width, out_cols)
        result = None
        for h in range(NX):
            term = jnp.dot(
                att[i, h].reshape(NX * part, g_width),
                weight[h * g_width : (h + 1) * g_width],
                preferred_element_type=jnp.float32,
            )
            result = term if result is None else result + term
        acc[...] = result
        for slot in (3, 2, 1, 0):
            j = xs(deltas[slot])
            kept = xg[slot, i * part : (i + 1) * part, own_cols].astype(jnp.float32)
            at = pl.ds(pl.multiple_of(j * part, part), part)
            obuf[i, slot] = (acc[at, :] + kept).astype(jnp.bfloat16)
            send(
                ("out", i, slot),
                lambda slot=slot: obuf.at[i, slot],
                (ps(1), y, j),
                lambda: out_part(i, 0),
            )

    def o_steps(step, pieces):
        if step < reach - 1:
            ring_step("o", step, pieces)

    attend(0, 0)
    ring_step("o", 0, ((0, -1),) + going_south)
    attend(0, 1)
    att_low(0)
    with jax.named_scope("attend0b"):
        attend(0, 2)
        attend(0, 3)
    att_high(0)
    with jax.named_scope("attend1a"):
        attend(1, 0)
        attend(1, 1)
    ring_step("o", 0, ((0, 1),) + going_north)
    o_steps(1, ((0, -1),) + going_south)
    with jax.named_scope("attend1b"):
        attend(1, 2)
        attend(1, 3)
    att_pass(0)
    att_start(1)
    o_steps(1, ((0, 1),) + going_north)
    for step in range(2, reach - 1):
        o_steps(step, ((0, -1),) + going_south)
    att_in(0)
    att_pass(1)
    for step in range(2, reach - 1):
        o_steps(step, ((0, 1),) + going_north)
    ring_step("o", reach - 1)
    with jax.named_scope("finish0"):
        finish(0)
    att_in(1)
    with jax.named_scope("finish1"):
        finish(1)
    with jax.named_scope("out_in"):
        for i in range(CHUNKS):
            for slot in (3, 2, 1, 0):
                land(("out", i, slot), out_part(i, -deltas[slot]))
    with jax.named_scope("wait_send"):
        for name, src in sources.items():
            copy_of(name, src(), src(), (p, y, x)).wait_send()


def body(states, norm_gain, w_in, w_out, lengths):
    rows, depth = states.shape[1:]
    w_rows = w_in.shape[1]
    o_rows = w_out.shape[1]
    out_cols = depth // NX
    n_pipe = lax.axis_size("pipe")
    n_y = lax.axis_size("ctx_y")
    part = rows // CHUNKS
    copies = 160
    bf16, f32 = jnp.bfloat16, jnp.float32
    moved = pl.pallas_call(
        functools.partial(tick_kernel, n_pipe, n_y),
        out_shape=pltpu.VMEM((rows, depth), bf16),
        in_specs=[
            pl.BlockSpec(memory_space=pl.ANY),
            pl.BlockSpec(memory_space=pl.ANY),
            pl.BlockSpec(memory_space=pl.ANY),
            pl.BlockSpec(memory_space=pl.ANY),
            pl.BlockSpec(memory_space=pl.ANY),
        ],
        out_specs=pl.BlockSpec(memory_space=pltpu.VMEM),
        scratch_shapes=[
            pltpu.SMEM(lengths.shape[::-1], jnp.int32),
            pltpu.VMEM((1, depth), f32),
            pltpu.VMEM((4, rows, depth), bf16),
            pltpu.VMEM((4 * rows, depth), bf16),
            pltpu.VMEM((w_rows, w_in.shape[2]), bf16),
            pltpu.VMEM((NX, w_rows, 128), bf16),
            pltpu.VMEM((n_y, NX, w_rows, 128), bf16),
            pltpu.VMEM((n_y, NX, w_rows, GROUP * HEAD_DIM), bf16),
            pltpu.VMEM((n_y, NX, o_rows, out_cols), bf16),
            pltpu.VMEM((4, 2, rows, 128), f32),
            pltpu.VMEM((CHUNKS, NX, part, WINDOW * rows), f32),
            pltpu.VMEM((NX, GROUP, rows, 128), bf16),
            pltpu.VMEM((3 * NX, rows, 128), bf16),
            pltpu.VMEM((3 * NX, rows, 128), bf16),
            pltpu.VMEM((CHUNKS, NX, NX, part, GROUP * HEAD_DIM), bf16),
            pltpu.VMEM((NX * part, out_cols), f32),
            pltpu.VMEM((CHUNKS, 4, part, out_cols), bf16),
            pltpu.SemaphoreType.DMA((5,)),
            pltpu.SemaphoreType.DMA((copies,)),
            pltpu.SemaphoreType.DMA((copies,)),
        ],
        compiler_params=pltpu.CompilerParams(
            collective_id=0, has_side_effects=True, vmem_limit_bytes=60 * 1024 * 1024
        ),
        name="tick",
    )(lengths.T, norm_gain, states[0], w_in[0], w_out[0])
    return moved[None]


def solution(mesh):
    n_pipe = mesh.shape["pipe"]
    n_y = mesh.shape["ctx"] // NX
    finer = Mesh(mesh.devices.reshape(n_pipe, n_y, NX), ("pipe", "ctx_y", "ctx_x"))
    ctx = ("ctx_y", "ctx_x")
    placed = (
        P("pipe", ctx, None),
        P("pipe", None),
        P("pipe", ctx, None),
        P("pipe", ctx, None),
        P(),
    )
    return jax.shard_map(
        body, mesh=finer, in_specs=placed, out_specs=P("pipe", ctx, None), check_vma=False
    )
```
